256 devices in a mesh: shard: 16 (over z, core), cols: 4 (over y), job: 4 (over x).
Axes of the slice: x: 4, y: 4, z: 8, core: 2. Of those that a mesh axis runs over, the one named last changes fastest.
Arguments:
- one_query: float32 [16384, 4096], P(('job', 'shard'), 'cols'), parts along dimension 0, may hold values from -0.125 to 0.125
- other_query: float32 [16384, 4096], P(('job', 'shard'), 'cols'), parts along dimension 0, may hold values from -0.09375 to 0.09375
- one_key: float32 [16384, 1024], P(('job', 'shard'), 'cols'), parts along dimension 0, may hold values from -0.125 to 0.125
- other_key: float32 [16384, 1024], P(('job', 'shard'), 'cols'), parts along dimension 0, may hold values from -0.09375 to 0.09375
- one_value: float32 [16384, 1024], P(('job', 'shard'), 'cols'), parts along dimension 0, may hold values from -0.125 to 0.125
- other_value: float32 [16384, 1024], P(('job', 'shard'), 'cols'), parts along dimension 0, may hold values from -0.09375 to 0.09375
- mix_share: float32 [16384], P(('job', 'shard')), parts along dimension 0, may hold values from 0.2 to 0.8
- norm_gain: float32 [16384], P(('job', 'shard')), parts along dimension 0, may hold values from 0.25 to 1.75
Outputs:
- final_query: bfloat16 [16384, 4096], P('job', 'cols'), parts along dimension 0
- final_key: bfloat16 [16384, 1024], P('job', 'cols'), parts along dimension 0
- final_value: bfloat16 [16384, 1024], P('job', 'cols'), parts along dimension 0
- scale_query: float32 [16384], P(('job', 'cols')), parts along dimension 0
- scale_key: float32 [4096], P(('job', 'cols')), parts along dimension 0
- scale_value: float32 [4096], P(('job', 'cols')), parts along dimension 0
The draws below stay inside these ranges and needn't reach their ends.
There are 4 independent parts, one for each index of `job`. The reference program is written for one: setup_inputs(seed, part) draws one part's arguments, and reference() takes and returns one part's arrays. A program takes and returns all parts, laid end to end along the dimension named above; each array names one. Nothing has to cross between parts.
All inputs are finite; a program needn't handle non-finite values. Where the reference program divides by a largest or mean magnitude, that divisor is 1e-20 or more.
Results may differ from the reference program's by a relative error of at most 0.001.
Values may be sent and summed in bfloat16 or wider, within the bound.
A program may use at most 128 MiB of HBM per device.

```python
import jax
import jax.numpy as jnp

D_MODEL = 4096
Q_DIM = 4096
KV_DIM = 1024


def strengthened(drawn, rng, source, target, blocks, factor):
    def block_of(position):
        return (jnp.arange(drawn.shape[position]) // (drawn.shape[position] // blocks)).reshape((-1,) + (1,) * (drawn.ndim - 1 - position))

    one_side = jax.random.permutation(rng, blocks)[block_of(target)]
    second = (block_of(target) + blocks // 2) % blocks
    return jnp.where((block_of(source) == one_side) | (block_of(source) == second), factor * drawn, drawn)


def level_of(own_key, shape, shards, smallest, high):
    def one(position, blocks):
        steps = jax.random.uniform(jax.random.fold_in(jax.random.fold_in(own_key, 6), position), (blocks,), jnp.float32, smallest / len(shards), high / len(shards))
        return jnp.repeat(jnp.exp(steps), shape[position] // blocks).reshape((-1,) + (1,) * (len(shape) - position - 1))

    factor_of = one(*shards[0])
    for cut in shards[1:]:
        factor_of = factor_of * one(*cut)
    return factor_of


def normal_values(key, shape, width, most, cuts=(), dtype=jnp.bfloat16):
    array = width * jax.random.normal(key, shape, jnp.float32)
    if cuts:
        array = array * level_of(key, shape, cuts, -0.22, 0.18)
    return jnp.clip(array, -most, most).astype(dtype)


def noise_with(stream_key, shape, scale, bound, pieces, heavy, dtype=jnp.bfloat16):
    entries = scale * jax.random.normal(stream_key, shape, jnp.float32)
    if pieces:
        entries = entries * level_of(stream_key, shape, pieces, -0.22, 0.18)
    return jnp.clip(strengthened(entries, jax.random.fold_in(stream_key, 3), *heavy), -bound, bound).astype(dtype)


def setup_inputs(seed: int = 0, part: int = 0) -> dict:
    arg_keys = jax.random.split(jax.random.key(seed), 9)
    part_keys = jax.random.split(jax.random.fold_in(arg_keys[8], part), 9)
    return {
        "one_query": noise_with(part_keys[0], (D_MODEL, Q_DIM), D_MODEL ** -0.5, 0.125, ((0, 16), (1, 4)), (0, 1, 16, 2.0), jnp.float32),
        "other_query": normal_values(part_keys[1], (D_MODEL, Q_DIM), D_MODEL ** -0.5, 0.09375, ((0, 16), (1, 4)), jnp.float32),
        "one_key": noise_with(part_keys[2], (D_MODEL, KV_DIM), D_MODEL ** -0.5, 0.125, ((0, 16), (1, 4)), (0, 1, 16, 2.0), jnp.float32),
        "other_key": normal_values(part_keys[3], (D_MODEL, KV_DIM), D_MODEL ** -0.5, 0.09375, ((0, 16), (1, 4)), jnp.float32),
        "one_value": noise_with(part_keys[4], (D_MODEL, KV_DIM), D_MODEL ** -0.5, 0.125, ((0, 16), (1, 4)), (0, 1, 16, 2.0), jnp.float32),
        "other_value": normal_values(part_keys[5], (D_MODEL, KV_DIM), D_MODEL ** -0.5, 0.09375, ((0, 16), (1, 4)), jnp.float32),
        "mix_share": jnp.clip(0.2 + 0.6 * jax.random.uniform(part_keys[6], (D_MODEL,), jnp.float32) ** level_of(part_keys[6], (D_MODEL,), ((0, 16),), -0.2, 0.2), 0.2, 0.8),
        "norm_gain": jnp.clip(1.0 + 0.15 * jax.random.normal(part_keys[7], (D_MODEL,), jnp.float32), 0.25, 1.75),
    }


def reference(one_query, other_query, one_key, other_key, one_value, other_value, mix_share, norm_gain):
    result_query = mix_share[:, None] * one_query + (1.0 - mix_share[:, None]) * other_query
    result_key = mix_share[:, None] * one_key + (1.0 - mix_share[:, None]) * other_key
    result_value = mix_share[:, None] * one_value + (1.0 - mix_share[:, None]) * other_value
    result_gained_query = result_query * norm_gain[:, None]
    result_gained_key = result_key * norm_gain[:, None]
    result_gained_value = result_value * norm_gain[:, None]
    scale_query = jnp.max(jnp.abs(result_gained_query), axis=0)
    final_query = (result_gained_query / scale_query).astype(jnp.bfloat16)
    scale_key = jnp.max(jnp.abs(result_gained_key), axis=0)
    final_key = (result_gained_key / scale_key).astype(jnp.bfloat16)
    scale_value = jnp.max(jnp.abs(result_gained_value), axis=0)
    final_value = (result_gained_value / scale_value).astype(jnp.bfloat16)
    return final_query, final_key, final_value, scale_query, scale_key, scale_value
```

```python
import functools

import jax
import jax.numpy as jnp
from jax import lax
from jax.experimental import pallas as pl
from jax.experimental.pallas import tpu as pltpu
from jax.sharding import PartitionSpec as P

MESH = pl.DeviceIdType.MESH
PARTS = 4


def kernel(
    n,
    one_query,
    other_query,
    one_key,
    other_key,
    one_value,
    other_value,
    mix_share,
    norm_gain,
    query,
    key,
    value,
    scale_query,
    scale_key,
    scale_value,
    ins,
    mix_rows,
    gained,
    maxima,
    load_sem,
    max_send,
    max_recv,
    right_send,
    right_recv,
    left_send,
    left_recv,
    side_send,
    side_recv,
):
    one_q, other_q, one_k, other_k, one_v, other_v, share, gain = ins
    mix_a, mix_b = mix_rows
    gained_q, gained_k, gained_v = gained
    rows, wide = one_query.shape
    narrow = one_key.shape[1]
    chips = n // 2
    me = lax.axis_index("shard")
    core = lax.rem(me, 2)
    sibling = me + 1 - 2 * core
    right, left = lax.rem(me + 2, n), lax.rem(me + n - 2, n)

    loads = [
        pltpu.make_async_copy(src, dst, load_sem.at[i])
        for i, (src, dst) in enumerate(
            [
                (mix_share, share),
                (norm_gain, gain),
                (one_key, one_k),
                (other_key, other_k),
                (one_value, one_v),
                (other_value, other_v),
                (one_query, one_q),
                (other_query, other_q),
            ]
        )
    ]
    for load in loads:
        load.start()
    barrier = pltpu.get_barrier_semaphore()
    for d in range(1, n):
        pl.semaphore_signal(
            barrier, inc=1, device_id={"shard": lax.rem(me + d, n)}, device_id_type=MESH
        )

    loads[0].wait()
    loads[1].wait()
    for t in range(rows // 128):
        at = pl.ds(128 * t, 128)
        m = jnp.broadcast_to(share[at].reshape(1, 128), (128, 128)).T
        g = jnp.broadcast_to(gain[at].reshape(1, 128), (128, 128)).T
        mix_a[at, :] = m * g
        mix_b[at, :] = (1.0 - m) * g

    def mixed(one, other, out, first, columns):
        for t in range(columns // 128):
            at = pl.ds(128 * t, 128)
            x = mix_a[...] * one[:, at] + mix_b[...] * other[:, at]
            out[:, at] = x
            maxima[0, :, pl.ds(first + 128 * t, 128)] = jnp.max(
                jnp.abs(x), axis=0, keepdims=True
            )

    loads[2].wait()
    loads[3].wait()
    mixed(one_k, other_k, gained_k, wide, narrow)
    loads[4].wait()
    loads[5].wait()
    mixed(one_v, other_v, gained_v, wide + narrow, narrow)
    loads[6].wait()
    loads[7].wait()
    mixed(one_q, other_q, gained_q, 0, wide)

    pl.semaphore_wait(barrier, n - 1)
    sends = []
    for d in sorted(range(1, n), key=lambda d: -min(d, n - d)):
        copy = pltpu.make_async_remote_copy(
            src_ref=maxima.at[0],
            dst_ref=maxima.at[d],
            send_sem=max_send.at[d],
            recv_sem=max_recv.at[d],
            device_id={"shard": lax.rem(me + d, n)},
            device_id_type=MESH,
        )
        copy.start()
        sends.append(copy)
    for copy in sends:
        copy.wait_recv()
    top = maxima[0]
    for d in range(1, n):
        top = jnp.maximum(top, maxima[d])
    over = 1.0 / top

    chunks = PARTS + 2
    part = rows // PARTS

    def place(owner, k):
        first = owner * rows
        if k < PARTS:
            return query.at[pl.ds(pl.multiple_of(first + k * part, part), part), :]
        out = key if k == PARTS else value
        return out.at[pl.ds(pl.multiple_of(first, rows), rows), :]

    def passed(ref, device, send_sem, recv_sem):
        return pltpu.make_async_remote_copy(
            src_ref=ref,
            dst_ref=ref,
            send_sem=send_sem,
            recv_sem=recv_sem,
            device_id={"shard": device},
            device_id_type=MESH,
        )

    ways = [
        (right, -2, right_send, right_recv, [k for k in range(chunks) if k % 2 == 0]),
        (left, 2, left_send, left_recv, [k for k in range(chunks) if k % 2 == 1]),
    ]
    steps = chips // 2
    started = []

    def onward(way, step, k):
        device, back, send_sem, recv_sem, last = ways[way]
        if step < steps - 1 or (step == steps - 1 and k in last):
            ref = place(lax.rem(me + back * step + 2 * n, n), k)
            copy = passed(ref, device, send_sem.at[step, k], recv_sem.at[step, k])
            copy.start()
            started.append(copy)

    def aside(slot, owner, k):
        copy = passed(place(owner, k), sibling, side_send.at[slot, k], side_recv.at[slot, k])
        copy.start()
        started.append(copy)
        beside.append((slot, owner, k))

    beside = []
    for k in range(chunks):
        if k < PARTS:
            x = gained_q[pl.ds(k * part, part), :] * over[:, :wide]
        elif k == PARTS:
            x = gained_k[...] * over[:, wide : wide + narrow]
        else:
            x = gained_v[...] * over[:, wide + narrow :]
        place(me, k)[...] = x.astype(jnp.bfloat16)
        onward(0, 0, k)
        onward(1, 0, k)
        aside(0, me, k)
    scale_query[...] = top[0, :wide]
    scale_key[...] = top[0, wide : wide + narrow]
    scale_value[...] = top[0, wide + narrow :]

    for step in range(steps):
        for k in range(chunks):
            for way, (device, back, send_sem, recv_sem, last) in enumerate(ways):
                if step == steps - 1 and k not in last:
                    continue
                owner = lax.rem(me + back * (step + 1) + 2 * n, n)
                passed(
                    place(owner, k), device, send_sem.at[step, k], recv_sem.at[step, k]
                ).wait_recv()
                onward(way, step + 1, k)
                slot = 1 + 2 * step + (way if step < steps - 1 else 0)
                aside(slot, owner, k)

    for slot, owner, k in beside:
        theirs = owner + 1 - 2 * core
        passed(
            place(theirs, k), sibling, side_send.at[slot, k], side_recv.at[slot, k]
        ).wait_recv()
    for copy in sends + started:
        copy.wait_send()


def stored(*refs):
    count = len(refs) // 2
    sems = refs[-1]
    copies = [
        pltpu.make_async_copy(src, dst, sems.at[i])
        for i, (src, dst) in enumerate(zip(refs[:count], refs[count:-1]))
    ]
    for copy in copies:
        copy.start()
    for copy in copies:
        copy.wait()


def shards(
    one_query, other_query, one_key, other_key, one_value, other_value, mix_share, norm_gain
):
    n = lax.axis_size("shard")
    rows, wide = one_query.shape
    narrow = one_key.shape[1]
    chunks, steps = PARTS + 2, n // 4
    full = (rows, wide), (rows, wide), (rows, narrow), (rows, narrow), (rows, narrow), (rows, narrow)
    hbm = pl.BlockSpec(memory_space=pltpu.HBM)
    vmem = pl.BlockSpec(memory_space=pltpu.VMEM)
    outs = [
        pltpu.VMEM(shape, dtype)
        for shape, dtype in [
            ((n * rows, wide), jnp.bfloat16),
            ((n * rows, narrow), jnp.bfloat16),
            ((n * rows, narrow), jnp.bfloat16),
            ((wide,), jnp.float32),
            ((narrow,), jnp.float32),
            ((narrow,), jnp.float32),
        ]
    ]
    whole = pl.pallas_call(
        functools.partial(kernel, n),
        out_shape=outs,
        in_specs=[hbm] * 8,
        out_specs=[vmem] * 6,
        scratch_shapes=[
            tuple(pltpu.VMEM(shape, jnp.float32) for shape in full)
            + (pltpu.VMEM((rows,), jnp.float32),) * 2,
            (pltpu.VMEM((rows, 128), jnp.float32),) * 2,
            tuple(pltpu.VMEM(shape, jnp.float32) for shape in full[::2]),
            pltpu.VMEM((n, 1, wide + 2 * narrow), jnp.float32),
            pltpu.SemaphoreType.DMA((8,)),
            pltpu.SemaphoreType.DMA((n,)),
            pltpu.SemaphoreType.DMA((n,)),
            pltpu.SemaphoreType.DMA((steps, chunks)),
            pltpu.SemaphoreType.DMA((steps, chunks)),
            pltpu.SemaphoreType.DMA((steps, chunks)),
            pltpu.SemaphoreType.DMA((steps, chunks)),
            pltpu.SemaphoreType.DMA((n // 2, chunks)),
            pltpu.SemaphoreType.DMA((n // 2, chunks)),
        ],
        compiler_params=pltpu.CompilerParams(
            collective_id=0, has_side_effects=True, vmem_limit_bytes=24 * 2**20
        ),
    )(
        *(
            pltpu.with_memory_space_constraint(x, pltpu.HBM)
            for x in (
                one_query,
                other_query,
                one_key,
                other_key,
                one_value,
                other_value,
                mix_share,
                norm_gain,
            )
        )
    )
    return pl.pallas_call(
        stored,
        out_shape=[pltpu.HBM(x.shape, x.dtype) for x in whole],
        in_specs=[vmem] * 6,
        out_specs=[hbm] * 6,
        scratch_shapes=[pltpu.SemaphoreType.DMA((6,))],
        compiler_params=pltpu.CompilerParams(vmem_limit_bytes=2**20),
    )(*whole)


def solution(mesh):
    placed = (
        P(("job", "shard"), "cols"),
        P(("job", "shard"), "cols"),
        P(("job", "shard"), "cols"),
        P(("job", "shard"), "cols"),
        P(("job", "shard"), "cols"),
        P(("job", "shard"), "cols"),
        P(("job", "shard")),
        P(("job", "shard")),
    )
    return jax.shard_map(
        shards,
        mesh=mesh,
        in_specs=placed,
        out_specs=(
            P("job", "cols"),
            P("job", "cols"),
            P("job", "cols"),
            P(("job", "cols")),
            P(("job", "cols")),
            P(("job", "cols")),
        ),
        check_vma=False,
    )
```

```python
import functools

import jax
import jax.numpy as jnp
from jax import lax
from jax.experimental import pallas as pl
from jax.experimental.pallas import tpu as pltpu
from jax.sharding import PartitionSpec as P

MESH = pl.DeviceIdType.MESH
STORES = 2


def kernel(
    n,
    pieces,
    one_query,
    other_query,
    one_key,
    other_key,
    one_value,
    other_value,
    mix_share,
    norm_gain,
    whole,
    scale_query,
    scale_key,
    scale_value,
    ins,
    mix_a,
    mix_b,
    gained,
    maxima,
    load_sem,
    max_sem,
    send_sem,
    side_sem,
    right_recv,
    left_recv,
):
    one_q, other_q, one_k, other_k, one_v, other_v, share, gain = ins
    rows, wide = one_query.shape
    narrow = one_key.shape[1]
    chips = n // 2
    me = lax.axis_index("shard")
    core = lax.rem(me, 2)
    sibling = me + 1 - 2 * core
    right, left = lax.rem(me + 2, n), lax.rem(me + n - 2, n)

    barrier = pltpu.get_barrier_semaphore()
    for d in range(1, n):
        pl.semaphore_signal(
            barrier, inc=1, device_id={"shard": lax.rem(me + d, n)}, device_id_type=MESH
        )
    loads = [
        pltpu.make_async_copy(src, dst, load_sem.at[i])
        for i, (src, dst) in enumerate(
            [
                (mix_share, share),
                (norm_gain, gain),
                (one_key, one_k),
                (other_key, other_k),
                (one_value, one_v),
                (other_value, other_v),
                (one_query, one_q),
                (other_query, other_q),
            ]
        )
    ]
    for load in loads:
        load.start()

    loads[0].wait()
    loads[1].wait()
    for t in range(rows // 128):
        at = pl.ds(128 * t, 128)
        m = jnp.broadcast_to(share[at].reshape(1, 128), (128, 128)).T
        g = jnp.broadcast_to(gain[at].reshape(1, 128), (128, 128)).T
        mix_a[at, :] = m * g
        mix_b[at, :] = (1.0 - m) * g

    def mixed(one, other, first, columns):
        for t in range(columns // 128):
            at, to = pl.ds(128 * t, 128), pl.ds(first + 128 * t, 128)
            x = mix_a[...] * one[:, at] + mix_b[...] * other[:, at]
            gained[:, to] = x
            maxima[0, :, to] = jnp.max(jnp.abs(x), axis=0, keepdims=True)

    loads[2].wait()
    loads[3].wait()
    mixed(one_k, other_k, wide, narrow)
    loads[4].wait()
    loads[5].wait()
    mixed(one_v, other_v, wide + narrow, narrow)
    loads[6].wait()
    loads[7].wait()
    mixed(one_q, other_q, 0, wide)

    def sent(src, dst, device, send, recv):
        return pltpu.make_async_remote_copy(
            src_ref=src,
            dst_ref=dst,
            send_sem=send,
            recv_sem=recv,
            device_id={"shard": device},
            device_id_type=MESH,
        )

    pl.semaphore_wait(barrier, n - 1)
    for d in sorted(range(1, n), key=lambda d: -min(d, n - d)):
        sent(maxima.at[0], maxima.at[d], lax.rem(me + d, n), max_sem.at[0], max_sem.at[1]).start()
    others = maxima.at[pl.ds(1, n - 1)]
    all_maxima = sent(others, others, right, max_sem.at[0], max_sem.at[1])
    all_maxima.wait_recv()
    top = maxima[0]
    for d in range(1, n):
        top = jnp.maximum(top, maxima[d])
    over = 1.0 / top

    def place(owner, k):
        first, count = pieces[k]
        return whole.at[pl.ds(pl.multiple_of(owner * rows + first, 8), count), :]

    steps, count = chips // 2, len(pieces)
    ways = [
        (right, -2, right_recv, range(count // 2)),
        (left, 2, left_recv, range(count // 2, count)),
    ]

    def onward(way, step, k):
        device, back, recv, last = ways[way]
        if step < steps - 1 or (step == steps - 1 and k in last):
            ref = place(lax.rem(me + back * step + 2 * n, n), k)
            sent(ref, ref, device, send_sem.at[0], recv.at[step, k]).start()

    def aside(owner, k):
        ref = place(owner, k)
        sent(ref, ref, sibling, send_sem.at[0], side_sem.at[0]).start()

    for k, (first, many) in enumerate(pieces):
        x = gained[pl.ds(first, many), :] * over
        place(me, k)[...] = x.astype(jnp.bfloat16)
        onward(0, 0, k)
        onward(1, 0, k)
        aside(me, k)
    scale_query[...] = top[0, :wide]
    scale_key[...] = top[0, wide : wide + narrow]
    scale_value[...] = top[0, wide + narrow :]

    for step in range(steps):
        for k in range(count):
            for way, (device, back, recv, last) in enumerate(ways):
                if step == steps - 1 and k not in last:
                    continue
                owner = lax.rem(me + back * (step + 1) + 2 * n, n)
                ref = place(owner, k)
                sent(ref, ref, device, send_sem.at[0], recv.at[step, k]).wait_recv()
                onward(way, step + 1, k)
                aside(owner, k)

    theirs = whole.at[pl.ds(0, chips * rows), :]
    sent(theirs, theirs, sibling, send_sem.at[0], side_sem.at[0]).wait_recv()
    onwards = whole.at[pl.ds(0, (2 * chips - 1) * rows), :]
    sent(onwards, onwards, sibling, send_sem.at[0], side_sem.at[0]).wait_send()
    all_maxima.wait_send()


def stored(whole, one, two, three, query, key, value, scale_query, scale_key, scale_value, sems):
    length = whole.shape[0] // STORES
    at, copies = 0, []
    for out in (query, key, value):
        for p in range(STORES):
            part = pl.ds(p * length, length)
            copies.append((whole.at[part, pl.ds(at, out.shape[1])], out.at[part, :]))
        at += out.shape[1]
    copies += [(one, scale_query), (two, scale_key), (three, scale_value)]
    copies = [
        pltpu.make_async_copy(src, dst, sems.at[i]) for i, (src, dst) in enumerate(copies)
    ]
    for copy in copies:
        copy.start()
    for copy in copies:
        copy.wait()


def shards(
    one_query, other_query, one_key, other_key, one_value, other_value, mix_share, norm_gain
):
    n = lax.axis_size("shard")
    rows, wide = one_query.shape
    narrow = one_key.shape[1]
    width = wide + 2 * narrow
    quarter = rows // 4
    pieces = [(k * quarter, quarter) for k in range(4)]
    steps = n // 4
    full = [(rows, wide)] * 2 + [(rows, narrow)] * 4
    hbm = pl.BlockSpec(memory_space=pltpu.HBM)
    vmem = pl.BlockSpec(memory_space=pltpu.VMEM)
    scales = [((wide,), jnp.float32), ((narrow,), jnp.float32), ((narrow,), jnp.float32)]
    gathered = pl.pallas_call(
        functools.partial(kernel, n, pieces),
        out_shape=[pltpu.VMEM((n * rows, width), jnp.bfloat16)]
        + [pltpu.VMEM(shape, dtype) for shape, dtype in scales],
        in_specs=[hbm] * 8,
        out_specs=[vmem] * 4,
        scratch_shapes=[
            tuple(pltpu.VMEM(shape, jnp.float32) for shape in full)
            + (pltpu.VMEM((rows,), jnp.float32),) * 2,
            pltpu.VMEM((rows, 128), jnp.float32),
            pltpu.VMEM((rows, 128), jnp.float32),
            pltpu.VMEM((rows, width), jnp.float32),
            pltpu.VMEM((n, 1, width), jnp.float32),
            pltpu.SemaphoreType.DMA((8,)),
            pltpu.SemaphoreType.DMA((2,)),
            pltpu.SemaphoreType.DMA((1,)),
            pltpu.SemaphoreType.DMA((1,)),
            pltpu.SemaphoreType.DMA((steps, len(pieces))),
            pltpu.SemaphoreType.DMA((steps, len(pieces))),
        ],
        compiler_params=pltpu.CompilerParams(
            collective_id=0, has_side_effects=True, vmem_limit_bytes=24 * 2**20
        ),
    )(
        *(
            pltpu.with_memory_space_constraint(x, pltpu.HBM)
            for x in (
                one_query,
                other_query,
                one_key,
                other_key,
                one_value,
                other_value,
                mix_share,
                norm_gain,
            )
        )
    )
    outs = [((n * rows, wide), jnp.bfloat16)] + [((n * rows, narrow), jnp.bfloat16)] * 2 + scales
    return pl.pallas_call(
        stored,
        out_shape=[pltpu.HBM(shape, dtype) for shape, dtype in outs],
        in_specs=[vmem] * 4,
        out_specs=[hbm] * 6,
        scratch_shapes=[pltpu.SemaphoreType.DMA((3 * STORES + 3,))],
        compiler_params=pltpu.CompilerParams(vmem_limit_bytes=2**20),
    )(*gathered)


def solution(mesh):
    placed = (
        P(("job", "shard"), "cols"),
        P(("job", "shard"), "cols"),
        P(("job", "shard"), "cols"),
        P(("job", "shard"), "cols"),
        P(("job", "shard"), "cols"),
        P(("job", "shard"), "cols"),
        P(("job", "shard")),
        P(("job", "shard")),
    )
    return jax.shard_map(
        shards,
        mesh=mesh,
        in_specs=placed,
        out_specs=(
            P("job", "cols"),
            P("job", "cols"),
            P("job", "cols"),
            P(("job", "cols")),
            P(("job", "cols")),
            P(("job", "cols")),
        ),
        check_vma=False,
    )
```

```python
import functools

import jax
import jax.numpy as jnp
from jax import lax
from jax.experimental import pallas as pl
from jax.experimental.pallas import tpu as pltpu
from jax.sharding import PartitionSpec as P

MESH = pl.DeviceIdType.MESH
STORES = 2
AHEAD = 64


def kernel(
    n,
    pieces,
    one_query,
    other_query,
    one_key,
    other_key,
    one_value,
    other_value,
    mix_share,
    norm_gain,
    whole,
    scale_query,
    scale_key,
    scale_value,
    ins,
    mix_a,
    mix_b,
    gained,
    maxima,
    early,
    ahead,
    load_sem,
    max_sem,
    ahead_sem,
    send_sem,
    side_sem,
    right_recv,
    left_recv,
):
    one_q, other_q, one_k, other_k, one_v, other_v, share, gain = ins
    rows, wide = one_query.shape
    narrow = one_key.shape[1]
    chips, tiles = n // 2, (wide + 2 * narrow) // 128
    me = lax.axis_index("shard")
    core = lax.rem(me, 2)
    sibling = me + 1 - 2 * core
    right, left = lax.rem(me + 2, n), lax.rem(me + n - 2, n)

    chip = me // 2
    first, second = chip == 0, chip == 1
    barrier = pltpu.get_barrier_semaphore()
    for d in range(1, n):
        peer = lax.rem(me + d, n)

        @pl.when((peer // 2 != 1) | (chip <= 1))
        def _():
            pl.semaphore_signal(barrier, inc=1, device_id={"shard": peer}, device_id_type=MESH)

    blank = jnp.zeros(maxima.shape[1:], jnp.float32)

    @pl.when(second)
    def _():
        maxima[lax.rem(me - sibling + n, n)] = blank

    @pl.when(jnp.logical_not(second))
    def _():
        maxima[lax.rem(me - 2 + n, n)] = blank
        maxima[lax.rem(me - 3 + n, n)] = blank

    loads = [
        pltpu.make_async_copy(src, dst, load_sem.at[i])
        for i, (src, dst) in enumerate(
            [
                (mix_share, share),
                (norm_gain, gain),
                (one_key, one_k),
                (other_key, other_k),
                (one_value, one_v),
                (other_value, other_v),
                (one_query, one_q),
                (other_query, other_q),
            ]
        )
    ]
    for load in loads:
        load.start()

    loads[0].wait()
    loads[1].wait()
    for t in range(rows // 128):
        at = pl.ds(128 * t, 128)
        m = jnp.broadcast_to(share[at].reshape(1, 128), (128, 128)).T
        g = jnp.broadcast_to(gain[at].reshape(1, 128), (128, 128)).T
        mix_a[at, :] = m * g
        mix_b[at, :] = (1.0 - m) * g

    def mixed(one, other, first, columns):
        for t in range(columns // 128):
            at, to = pl.ds(128 * t, 128), pl.ds(first + 128 * t, 128)
            x = mix_a[...] * one[:, at] + mix_b[...] * other[:, at]
            gained[:, to] = x
            maxima[0, pl.ds(first // 128 + t, 1), :] = jnp.max(jnp.abs(x), axis=0, keepdims=True)

    loads[2].wait()
    loads[3].wait()
    mixed(one_k, other_k, wide, narrow)
    loads[4].wait()
    loads[5].wait()
    mixed(one_v, other_v, wide + narrow, narrow)
    loads[6].wait()
    loads[7].wait()
    mixed(one_q, other_q, 0, wide)

    def sent(src, dst, device, send, recv):
        return pltpu.make_async_remote_copy(
            src_ref=src,
            dst_ref=dst,
            send_sem=send,
            recv_sem=recv,
            device_id={"shard": device},
            device_id_type=MESH,
        )

    early_maxima = sent(maxima.at[0], early, left, max_sem.at[0], ahead_sem.at[0])
    early_rows = sent(gained.at[pl.ds(0, AHEAD), :], ahead, left, ahead_sem.at[1], ahead_sem.at[2])

    @pl.when(second)
    def _():
        pl.semaphore_wait(barrier, 3)
        early_maxima.start()
        early_rows.start()

    @pl.when(jnp.logical_not(second))
    def _():
        @pl.when(first)
        def _():
            early_maxima.wait_recv()
            maxima[0] = jnp.maximum(maxima[0], early[...])

        pl.semaphore_wait(barrier, n - 1)
        for d in sorted(range(1, n), key=lambda d: -min(d, n - d)):
            peer = lax.rem(me + d, n)
            sent(maxima.at[0], maxima.at[d], peer, max_sem.at[0], max_sem.at[1]).start()

    def heard(count):
        some = maxima.at[pl.ds(0, count)]
        return sent(some, some, right, max_sem.at[0], max_sem.at[1])

    @pl.when(second)
    def _():
        heard(n - 2).wait_recv()

    @pl.when(jnp.logical_not(second))
    def _():
        heard(n - 3).wait_recv()

    top = maxima[0]
    for d in range(1, n):
        top = jnp.maximum(top, maxima[d])
    over = 1.0 / top

    def place(owner, k):
        start, many = pieces[k]
        return whole.at[pl.ds(pl.multiple_of(owner * rows + start, 8), many), :]

    steps, count = chips // 2, len(pieces)
    ways = [(right, -2, right_recv, (0, 2, 4)), (left, 2, left_recv, (1, 3))]
    moved, early_piece = 2, 4

    def when(condition, run):
        if condition is True:
            run()
        elif condition is not False:
            pl.when(condition)(run)

    def goes(way, step, k, into_first):
        if step == steps - 1 and k == moved:
            return into_first if way == 1 else jnp.logical_not(into_first)
        if step == steps - 1:
            return k in ways[way][3]
        return step < steps

    def onward(way, step, k):
        device, back, recv, last = ways[way]

        def run():
            ref = place(lax.rem(me + back * step + 2 * n, n), k)
            sent(ref, ref, device, send_sem.at[0], recv.at[step, k]).start()

        condition = goes(way, step, k, second if way == 1 else chip == chips - 1)
        if way == 1 and step == 0 and k == early_piece:
            condition = jnp.logical_not(second)
        when(condition, run)

    def aside(owner, k):
        ref = place(owner, k)
        sent(ref, ref, sibling, send_sem.at[0], side_sem.at[0]).start()

    def scaled(rows_of, to):
        for t in range(tiles):
            at = pl.ds(128 * t, 128)
            to[:, at] = (rows_of[:, at] * over[t : t + 1, :]).astype(jnp.bfloat16)

    for k, (start, many) in enumerate(pieces):
        scaled(gained.at[pl.ds(start, many), :], place(me, k))
        onward(0, 0, k)
        onward(1, 0, k)
        aside(me, k)
    t = 0
    for out in (scale_query, scale_key, scale_value):
        for p in range(out.shape[0] // 128):
            out[pl.ds(128 * p, 128)] = top[t, :]
            t += 1

    for step in range(steps):
        for k in range(count):
            for way, (device, back, recv, last) in enumerate(ways):
                owner = lax.rem(me + back * (step + 1) + 2 * n, n)
                ref = place(owner, k)
                arrived = sent(ref, ref, device, send_sem.at[0], recv.at[step, k])
                if way == 1 and step == 0 and k == early_piece:

                    @pl.when(first)
                    def _():
                        early_rows.wait_recv()
                        scaled(ahead, ref)

                    pl.when(jnp.logical_not(first))(arrived.wait_recv)
                    onward(way, step + 1, k)
                    aside(owner, k)
                    continue

                def run():
                    arrived.wait_recv()
                    onward(way, step + 1, k)
                    aside(owner, k)

                when(goes(way, step, k, first), run)

    theirs = whole.at[pl.ds(0, chips * rows), :]
    sent(theirs, theirs, sibling, send_sem.at[0], side_sem.at[0]).wait_recv()
    def all_sent(count):
        onwards = whole.at[pl.ds(0, count), :]
        sent(onwards, onwards, sibling, send_sem.at[0], side_sem.at[0]).wait_send()

    everything, less = (2 * chips - 1) * rows, pieces[moved][1]

    @pl.when(second)
    def _():
        all_sent(everything + less - AHEAD)
        early_maxima.wait_send()
        early_rows.wait_send()

    @pl.when(jnp.logical_not(second))
    def _():
        heard(n - 1).wait_send()
        pl.when(chip == chips - 1)(lambda: all_sent(everything - less))
        pl.when(chip != chips - 1)(lambda: all_sent(everything))


def stored(whole, one, two, three, query, key, value, scale_query, scale_key, scale_value, sems):
    length = whole.shape[0] // STORES
    at, copies = 0, []
    for out in (query, key, value):
        for p in range(STORES):
            part = pl.ds(p * length, length)
            copies.append((whole.at[part, pl.ds(at, out.shape[1])], out.at[part, :]))
        at += out.shape[1]
    copies += [(one, scale_query), (two, scale_key), (three, scale_value)]
    copies = [
        pltpu.make_async_copy(src, dst, sems.at[max(0, i - 3 * STORES + 1)])
        for i, (src, dst) in enumerate(copies)
    ]
    for copy in copies:
        copy.start()
    pltpu.make_async_copy(whole, whole, sems.at[0]).wait()
    for copy in copies[3 * STORES :]:
        copy.wait()


def shards(
    one_query, other_query, one_key, other_key, one_value, other_value, mix_share, norm_gain
):
    n = lax.axis_size("shard")
    rows, wide = one_query.shape
    narrow = one_key.shape[1]
    width = wide + 2 * narrow
    half, small = rows // 2, 16
    turn = half - AHEAD // 2
    pieces = [
        (AHEAD, turn - AHEAD),
        (half, half - small),
        (turn, half - turn),
        (rows - small, small),
        (0, AHEAD),
    ]
    steps = n // 4
    full = [(rows, wide)] * 2 + [(rows, narrow)] * 4
    hbm = pl.BlockSpec(memory_space=pltpu.HBM)
    vmem = pl.BlockSpec(memory_space=pltpu.VMEM)
    scales = [((wide,), jnp.float32), ((narrow,), jnp.float32), ((narrow,), jnp.float32)]
    gathered = pl.pallas_call(
        functools.partial(kernel, n, pieces),
        out_shape=[pltpu.VMEM((n * rows, width), jnp.bfloat16)]
        + [pltpu.VMEM(shape, dtype) for shape, dtype in scales],
        in_specs=[hbm] * 8,
        out_specs=[vmem] * 4,
        scratch_shapes=[
            tuple(pltpu.VMEM(shape, jnp.float32) for shape in full)
            + (pltpu.VMEM((rows,), jnp.float32),) * 2,
            pltpu.VMEM((rows, 128), jnp.float32),
            pltpu.VMEM((rows, 128), jnp.float32),
            pltpu.VMEM((rows, width), jnp.float32),
            pltpu.VMEM((n, width // 128, 128), jnp.float32),
            pltpu.VMEM((width // 128, 128), jnp.float32),
            pltpu.VMEM((AHEAD, width), jnp.float32),
            pltpu.SemaphoreType.DMA((8,)),
            pltpu.SemaphoreType.DMA((2,)),
            pltpu.SemaphoreType.DMA((3,)),
            pltpu.SemaphoreType.DMA((1,)),
            pltpu.SemaphoreType.DMA((1,)),
            pltpu.SemaphoreType.DMA((steps, len(pieces))),
            pltpu.SemaphoreType.DMA((steps, len(pieces))),
        ],
        compiler_params=pltpu.CompilerParams(
            collective_id=0, has_side_effects=True, vmem_limit_bytes=24 * 2**20
        ),
    )(
        *(
            pltpu.with_memory_space_constraint(x, pltpu.HBM)
            for x in (
                one_query,
                other_query,
                one_key,
                other_key,
                one_value,
                other_value,
                mix_share,
                norm_gain,
            )
        )
    )
    outs = [((n * rows, wide), jnp.bfloat16)] + [((n * rows, narrow), jnp.bfloat16)] * 2 + scales
    return pl.pallas_call(
        stored,
        out_shape=[pltpu.HBM(shape, dtype) for shape, dtype in outs],
        in_specs=[vmem] * 4,
        out_specs=[hbm] * 6,
        scratch_shapes=[pltpu.SemaphoreType.DMA((4,))],
        compiler_params=pltpu.CompilerParams(vmem_limit_bytes=2**20),
    )(*gathered)


def solution(mesh):
    placed = (
        P(("job", "shard"), "cols"),
        P(("job", "shard"), "cols"),
        P(("job", "shard"), "cols"),
        P(("job", "shard"), "cols"),
        P(("job", "shard"), "cols"),
        P(("job", "shard"), "cols"),
        P(("job", "shard")),
        P(("job", "shard")),
    )
    return jax.shard_map(
        shards,
        mesh=mesh,
        in_specs=placed,
        out_specs=(
            P("job", "cols"),
            P("job", "cols"),
            P("job", "cols"),
            P(("job", "cols")),
            P(("job", "cols")),
            P(("job", "cols")),
        ),
        check_vma=False,
    )
```

```python
import functools

import jax
import jax.numpy as jnp
from jax import lax
from jax.experimental import pallas as pl
from jax.experimental.pallas import tpu as pltpu
from jax.sharding import PartitionSpec as P

MESH = pl.DeviceIdType.MESH
STORES = 2
AHEAD = 48


def kernel(
    n,
    pieces,
    turned,
    one_query,
    other_query,
    one_key,
    other_key,
    one_value,
    other_value,
    mix_share,
    norm_gain,
    whole,
    scale_query,
    scale_key,
    scale_value,
    ins,
    mix_a,
    mix_b,
    gained,
    maxima,
    far,
    merged,
    whole_top,
    ahead,
    load_sem,
    max_sem,
    ahead_sem,
    near_sem,
    send_sem,
    side_sem,
    right_recv,
    left_recv,
):
    one_q, other_q, one_k, other_k, one_v, other_v, share, gain = ins
    rows, wide = one_query.shape
    narrow = one_key.shape[1]
    chips, tiles = n // 2, (wide + 2 * narrow) // 128
    me = lax.axis_index("shard")
    core = lax.rem(me, 2)
    sibling = me + 1 - 2 * core
    right, left = lax.rem(me + 2, n), lax.rem(me + n - 2, n)

    chip, half = me // 2, n // 2
    early = chip < chips // 2
    late = jnp.logical_not(early)
    base = half * (me // half)
    barrier = pltpu.get_barrier_semaphore()

    def greet(device):
        pl.semaphore_signal(barrier, inc=1, device_id={"shard": device}, device_id_type=MESH)

    for d in range(1, half):
        greet(base + lax.rem(me + d, half))

    @pl.when(early)
    def _():
        for d in range(half):
            greet(half + d)

    loads = [
        pltpu.make_async_copy(src, dst, load_sem.at[i])
        for i, (src, dst) in enumerate(
            [
                (mix_share, share),
                (norm_gain, gain),
                (one_key, one_k),
                (other_key, other_k),
                (one_value, one_v),
                (other_value, other_v),
                (one_query, one_q),
                (other_query, other_q),
            ]
        )
    ]
    for load in loads:
        load.start()

    loads[0].wait()
    loads[1].wait()
    for t in range(rows // 128):
        at = pl.ds(128 * t, 128)
        m = jnp.broadcast_to(share[at].reshape(1, 128), (128, 128)).T
        g = jnp.broadcast_to(gain[at].reshape(1, 128), (128, 128)).T
        mix_a[at, :] = m * g
        mix_b[at, :] = (1.0 - m) * g

    def mixed(one, other, first, columns):
        for t in range(columns // 128):
            at, to = pl.ds(128 * t, 128), pl.ds(first + 128 * t, 128)
            x = mix_a[...] * one[:, at] + mix_b[...] * other[:, at]
            gained[:, to] = x
            maxima[0, pl.ds(first // 128 + t, 1), :] = jnp.max(jnp.abs(x), axis=0, keepdims=True)

    loads[2].wait()
    loads[3].wait()
    mixed(one_k, other_k, wide, narrow)
    loads[4].wait()
    loads[5].wait()
    mixed(one_v, other_v, wide + narrow, narrow)
    loads[6].wait()
    loads[7].wait()
    mixed(one_q, other_q, 0, wide)

    def sent(src, dst, device, send, recv):
        return pltpu.make_async_remote_copy(
            src_ref=src,
            dst_ref=dst,
            send_sem=send,
            recv_sem=recv,
            device_id={"shard": device},
            device_id_type=MESH,
        )

    lower, upper = chip == 0, chip == chips // 2 - 1
    to_right, to_left = chip < chips // 2 - 1, early & (chip > 0)
    from_left, from_right = to_left, to_right
    mine = maxima.at[0]

    def within(d):
        sent(
            mine, maxima.at[d], base + lax.rem(me + d, half), max_sem.at[0], max_sem.at[1]
        ).start()

    def heard(ref, count, recv):
        some = ref.at[pl.ds(0, count)]
        return sent(some, some, right, max_sem.at[0], recv)

    def merged_to(device):
        return sent(merged, merged, device, max_sem.at[4], max_sem.at[3])

    early_rows = gained.at[pl.ds(0, AHEAD), :]
    right_rows = sent(early_rows, ahead.at[0], right, ahead_sem.at[0], ahead_sem.at[2])
    left_rows = sent(early_rows, ahead.at[1], left, ahead_sem.at[1], ahead_sem.at[3])

    @pl.when(early)
    def _():
        pl.semaphore_wait(barrier, half - 1)
        for d in range(1, half):
            within(d)
        pl.when(to_right)(right_rows.start)
        pl.when(to_left)(left_rows.start)

    @pl.when(late)
    def _():
        pl.semaphore_wait(barrier, n - 1)
        close = core + (half - 2) * (1 - chip // (chips * 3 // 4))
        pl.semaphore_signal(near_sem, inc=1, device_id={"shard": close}, device_id_type=MESH)
        for d in sorted(range(half), key=lambda d: -min(d + 1, half - d)):
            peer = lax.rem(me + half // 2 + 1 + d, half)
            sent(mine, far.at[me - half], peer, max_sem.at[0], max_sem.at[2]).start()
        for d in range(1, half):
            within(d)

    heard(maxima, half - 1, max_sem.at[1]).wait_recv()
    top = maxima[0]
    for d in range(1, half):
        top = jnp.maximum(top, maxima[d])

    @pl.when(lower | upper)
    def _():
        merged[...] = top
        pl.semaphore_wait(near_sem, 2)

        @pl.when(lower)
        def _():
            merged_to(n - 2 + core).start()
            merged_to(n - 4 + core).start()

        @pl.when(upper)
        def _():
            merged_to(half + core).start()
            merged_to(half + 2 + core).start()

    whole_top[...] = top

    @pl.when(early)
    def _():
        heard(far, half, max_sem.at[2]).wait_recv()
        most = whole_top[...]
        for d in range(half):
            most = jnp.maximum(most, far[d])
        whole_top[...] = most

    @pl.when(late)
    def _():
        merged_to(right).wait_recv()
        whole_top[...] = jnp.maximum(whole_top[...], merged[...])

    top = whole_top[...]
    over = 1.0 / top

    def place(owner, k):
        start, many = pieces[k]
        return whole.at[pl.ds(pl.multiple_of(owner * rows + start, 8), many), :]

    steps, count = chips // 2, len(pieces)
    ways = [(right, -2, right_recv), (left, 2, left_recv)]

    def when(condition, run):
        if condition is True:
            run()
        elif condition is not False:
            pl.when(condition)(run)

    def any_of(chosen):
        condition = False
        for c in chosen:
            condition = (chip == c) | condition
        return condition if chosen else False

    def goes(way, step, k, shift):
        if step < steps - 1:
            return True
        if step == steps:
            return False
        to = 1 if way == 0 else -1
        takers = [c for c in range(chips) if (k in turned[c]) == (way == 0)]
        senders = [(c - shift * to) % chips for c in takers]
        return True if len(senders) == chips else any_of(senders)

    def onward(way, step, k):
        device, back, recv = ways[way]

        def run():
            ref = place(lax.rem(me + back * step + 2 * n, n), k)
            sent(ref, ref, device, send_sem.at[0], recv.at[step, k]).start()

        condition = goes(way, step, k, 1)
        if step == 0 and k == 0:
            condition = jnp.logical_not(to_left if way == 1 else to_right)
        when(condition, run)

    def aside(owner, k):
        ref = place(owner, k)
        sent(ref, ref, sibling, send_sem.at[0], side_sem.at[0]).start()

    def scaled(rows_of, to):
        for t in range(tiles):
            at = pl.ds(128 * t, 128)
            to[:, at] = (rows_of[:, at] * over[t : t + 1, :]).astype(jnp.bfloat16)

    for k, (start, many) in enumerate(pieces):
        scaled(gained.at[pl.ds(start, many), :], place(me, k))
        onward(0, 0, k)
        onward(1, 0, k)
        aside(me, k)
    t = 0
    for out in (scale_query, scale_key, scale_value):
        for p in range(out.shape[0] // 128):
            out[pl.ds(128 * p, 128)] = top[t, :]
            t += 1

    for step in range(steps):
        for k in range(count):
            for way, (device, back, recv) in enumerate(ways):
                owner = lax.rem(me + back * (step + 1) + 2 * n, n)
                ref = place(owner, k)
                arrived = sent(ref, ref, device, send_sem.at[0], recv.at[step, k])
                if step == 0 and k == 0:
                    came = from_left if way == 0 else from_right

                    @pl.when(came)
                    def _():
                        (right_rows if way == 0 else left_rows).wait_recv()
                        scaled(ahead.at[way], ref)

                    pl.when(jnp.logical_not(came))(arrived.wait_recv)
                    onward(way, step + 1, k)
                    aside(owner, k)
                    continue

                def run():
                    arrived.wait_recv()
                    onward(way, step + 1, k)
                    aside(owner, k)

                when(goes(way, step, k, 0), run)

    theirs = whole.at[pl.ds(0, chips * rows), :]
    sent(theirs, theirs, sibling, send_sem.at[0], side_sem.at[0]).wait_recv()
    by_right = [sum(pieces[k][1] for k in turned[c]) for c in range(chips)]
    totals = {}
    for c in range(chips):
        total = (2 * chips - 1) * rows + by_right[(c + 1) % chips] - by_right[c - 1]
        total -= AHEAD * ((c < chips // 2 - 1) + (0 < c < chips // 2))
        totals.setdefault(total, []).append(c)
    for total, chosen in totals.items():

        @pl.when(any_of(chosen))
        def _():
            onwards = whole.at[pl.ds(0, total), :]
            sent(onwards, onwards, sibling, send_sem.at[0], side_sem.at[0]).wait_send()

    @pl.when(early)
    def _():
        heard(maxima, half - 1, max_sem.at[1]).wait_send()
        pl.when(to_right)(right_rows.wait_send)
        pl.when(to_left)(left_rows.wait_send)

    @pl.when(late)
    def _():
        both = maxima.at[pl.ds(0, n - 1)]
        sent(both, both, right, max_sem.at[0], max_sem.at[1]).wait_send()

    @pl.when(lower | upper)
    def _():
        both = maxima.at[pl.ds(0, 2)]
        sent(both, both, right, max_sem.at[4], max_sem.at[3]).wait_send()


def stored(whole, one, two, three, query, key, value, scale_query, scale_key, scale_value, sems):
    length = whole.shape[0] // STORES
    at, copies = 0, []
    for out in (query, key, value):
        for p in range(STORES):
            part = pl.ds(p * length, length)
            copies.append((whole.at[part, pl.ds(at, out.shape[1])], out.at[part, :]))
        at += out.shape[1]
    copies += [(one, scale_query), (two, scale_key), (three, scale_value)]
    copies = [
        pltpu.make_async_copy(src, dst, sems.at[max(0, i - 3 * STORES + 1)])
        for i, (src, dst) in enumerate(copies)
    ]
    for copy in copies:
        copy.start()
    pltpu.make_async_copy(whole, whole, sems.at[0]).wait()
    for copy in copies[3 * STORES :]:
        copy.wait()


def shards(
    one_query, other_query, one_key, other_key, one_value, other_value, mix_share, norm_gain
):
    n = lax.axis_size("shard")
    rows, wide = one_query.shape
    narrow = one_key.shape[1]
    width = wide + 2 * narrow
    middle, small = rows // 2, 16
    moved = AHEAD // 2
    pieces = [
        (0, AHEAD),
        (middle + moved, middle - moved - small),
        (AHEAD, middle - moved - AHEAD),
        (middle, moved),
        (middle - moved, moved),
        (rows - small, small),
    ]
    chips = n // 2
    turned = [(0, 2, 4)] * chips
    turned[0] = (0, 2)
    turned[chips // 2 - 1] = (0, 2, 3, 4)
    turned[chips // 2] = (0, 2)
    turned[chips - 1] = (0, 2, 3, 4)
    steps = n // 4
    full = [(rows, wide)] * 2 + [(rows, narrow)] * 4
    hbm = pl.BlockSpec(memory_space=pltpu.HBM)
    vmem = pl.BlockSpec(memory_space=pltpu.VMEM)
    scales = [((wide,), jnp.float32), ((narrow,), jnp.float32), ((narrow,), jnp.float32)]
    gathered = pl.pallas_call(
        functools.partial(kernel, n, pieces, turned),
        out_shape=[pltpu.VMEM((n * rows, width), jnp.bfloat16)]
        + [pltpu.VMEM(shape, dtype) for shape, dtype in scales],
        in_specs=[hbm] * 8,
        out_specs=[vmem] * 4,
        scratch_shapes=[
            tuple(pltpu.VMEM(shape, jnp.float32) for shape in full)
            + (pltpu.VMEM((rows,), jnp.float32),) * 2,
            pltpu.VMEM((rows, 128), jnp.float32),
            pltpu.VMEM((rows, 128), jnp.float32),
            pltpu.VMEM((rows, width), jnp.float32),
            pltpu.VMEM((n, width // 128, 128), jnp.float32),
            pltpu.VMEM((n // 2, width // 128, 128), jnp.float32),
            pltpu.VMEM((width // 128, 128), jnp.float32),
            pltpu.VMEM((width // 128, 128), jnp.float32),
            pltpu.VMEM((2, AHEAD, width), jnp.float32),
            pltpu.SemaphoreType.DMA((8,)),
            pltpu.SemaphoreType.DMA((5,)),
            pltpu.SemaphoreType.DMA((4,)),
            pltpu.SemaphoreType.REGULAR,
            pltpu.SemaphoreType.DMA((1,)),
            pltpu.SemaphoreType.DMA((1,)),
            pltpu.SemaphoreType.DMA((steps, len(pieces))),
            pltpu.SemaphoreType.DMA((steps, len(pieces))),
        ],
        compiler_params=pltpu.CompilerParams(
            collective_id=0, has_side_effects=True, vmem_limit_bytes=24 * 2**20
        ),
    )(
        *(
            pltpu.with_memory_space_constraint(x, pltpu.HBM)
            for x in (
                one_query,
                other_query,
                one_key,
                other_key,
                one_value,
                other_value,
                mix_share,
                norm_gain,
            )
        )
    )
    outs = [((n * rows, wide), jnp.bfloat16)] + [((n * rows, narrow), jnp.bfloat16)] * 2 + scales
    return pl.pallas_call(
        stored,
        out_shape=[pltpu.HBM(shape, dtype) for shape, dtype in outs],
        in_specs=[vmem] * 4,
        out_specs=[hbm] * 6,
        scratch_shapes=[pltpu.SemaphoreType.DMA((4,))],
        compiler_params=pltpu.CompilerParams(vmem_limit_bytes=2**20),
    )(*gathered)


def solution(mesh):
    placed = (
        P(("job", "shard"), "cols"),
        P(("job", "shard"), "cols"),
        P(("job", "shard"), "cols"),
        P(("job", "shard"), "cols"),
        P(("job", "shard"), "cols"),
        P(("job", "shard"), "cols"),
        P(("job", "shard")),
        P(("job", "shard")),
    )
    return jax.shard_map(
        shards,
        mesh=mesh,
        in_specs=placed,
        out_specs=(
            P("job", "cols"),
            P("job", "cols"),
            P("job", "cols"),
            P(("job", "cols")),
            P(("job", "cols")),
            P(("job", "cols")),
        ),
        check_vma=False,
    )
```

```python
import functools

import jax
import jax.numpy as jnp
from jax import lax
from jax.experimental import pallas as pl
from jax.experimental.pallas import tpu as pltpu
from jax.sharding import PartitionSpec as P

MESH = pl.DeviceIdType.MESH
STORES = 2
AHEAD = 48


def kernel(
    n,
    pieces,
    turned,
    one_query,
    other_query,
    one_key,
    other_key,
    one_value,
    other_value,
    mix_share,
    norm_gain,
    whole,
    scale_query,
    scale_key,
    scale_value,
    ins,
    mix_a,
    mix_b,
    gained,
    maxima,
    far,
    merged,
    whole_top,
    ahead,
    load_sem,
    max_sem,
    ahead_sem,
    near_sem,
    send_sem,
    side_sem,
    right_recv,
    left_recv,
):
    one_q, other_q, one_k, other_k, one_v, other_v, share, gain = ins
    rows, wide = one_query.shape
    narrow = one_key.shape[1]
    chips, tiles = n // 2, (wide + 2 * narrow) // 128
    me = lax.axis_index("shard")
    core = lax.rem(me, 2)
    sibling = me + 1 - 2 * core
    right, left = lax.rem(me + 2, n), lax.rem(me + n - 2, n)

    chip, half = me // 2, n // 2
    early = chip < chips // 2
    late = jnp.logical_not(early)
    base = half * (me // half)
    barrier = pltpu.get_barrier_semaphore()

    def greet(device):
        pl.semaphore_signal(barrier, inc=1, device_id={"shard": device}, device_id_type=MESH)

    for d in range(1, half):
        greet(base + lax.rem(me + d, half))

    @pl.when(early)
    def _():
        for d in range(half):
            greet(half + d)

    loads = [
        pltpu.make_async_copy(src, dst, load_sem.at[i])
        for i, (src, dst) in enumerate(
            [
                (mix_share, share),
                (norm_gain, gain),
                (one_key, one_k),
                (other_key, other_k),
                (one_value, one_v),
                (other_value, other_v),
                (one_query, one_q),
                (other_query, other_q),
            ]
        )
    ]
    for load in loads:
        load.start()

    loads[0].wait()
    loads[1].wait()
    for t in range(rows // 128):
        at = pl.ds(128 * t, 128)
        m = jnp.broadcast_to(share[at].reshape(1, 128), (128, 128)).T
        g = jnp.broadcast_to(gain[at].reshape(1, 128), (128, 128)).T
        mix_a[at, :] = m * g
        mix_b[at, :] = (1.0 - m) * g

    def mixed(one, other, first, columns):
        for t in range(columns // 128):
            at, to = pl.ds(128 * t, 128), pl.ds(first + 128 * t, 128)
            x = mix_a[...] * one[:, at] + mix_b[...] * other[:, at]
            gained[:, to] = x
            maxima[0, pl.ds(first // 128 + t, 1), :] = jnp.max(jnp.abs(x), axis=0, keepdims=True)

    loads[2].wait()
    loads[3].wait()
    mixed(one_k, other_k, wide, narrow)
    loads[4].wait()
    loads[5].wait()
    mixed(one_v, other_v, wide + narrow, narrow)
    loads[6].wait()
    loads[7].wait()
    mixed(one_q, other_q, 0, wide)

    def sent(src, dst, device, send, recv):
        return pltpu.make_async_remote_copy(
            src_ref=src,
            dst_ref=dst,
            send_sem=send,
            recv_sem=recv,
            device_id={"shard": device},
            device_id_type=MESH,
        )

    lower, upper = chip == 0, chip == chips // 2 - 1
    to_right, to_left = chip < chips // 2 - 1, early & (chip > 0)
    from_left, from_right = to_left, to_right
    mine = maxima.at[0]

    def within(d):
        sent(
            mine, maxima.at[d], base + lax.rem(me + d, half), max_sem.at[0], max_sem.at[1]
        ).start()

    def heard(ref, count, recv):
        some = ref.at[pl.ds(0, count)]
        return sent(some, some, right, max_sem.at[0], recv)

    def merged_to(device):
        return sent(merged, merged, device, max_sem.at[4], max_sem.at[3])

    early_rows = gained.at[pl.ds(0, AHEAD), :]
    right_rows = sent(early_rows, ahead.at[0], right, ahead_sem.at[0], ahead_sem.at[2])
    left_rows = sent(early_rows, ahead.at[1], left, ahead_sem.at[1], ahead_sem.at[3])

    @pl.when(early)
    def _():
        pl.semaphore_wait(barrier, half - 1)
        for d in range(1, half):
            within(d)
        pl.when(to_right)(right_rows.start)
        pl.when(to_left)(left_rows.start)

    @pl.when(late)
    def _():
        pl.semaphore_wait(barrier, n - 1)
        close = core + (half - 2) * (1 - chip // (chips * 3 // 4))
        pl.semaphore_signal(near_sem, inc=1, device_id={"shard": close}, device_id_type=MESH)
        for d in sorted(range(half), key=lambda d: -min(d + 1, half - d)):
            peer = lax.rem(me + half // 2 + 1 + d, half)
            sent(mine, far.at[me - half], peer, max_sem.at[0], max_sem.at[2]).start()
        for d in range(1, half):
            within(d)

    heard(maxima, half - 1, max_sem.at[1]).wait_recv()
    top = maxima[0]
    for d in range(1, half):
        top = jnp.maximum(top, maxima[d])

    @pl.when(lower | upper)
    def _():
        merged[...] = top
        pl.semaphore_wait(near_sem, 2)

        @pl.when(lower)
        def _():
            merged_to(n - 2 + core).start()
            merged_to(n - 4 + core).start()

        @pl.when(upper)
        def _():
            merged_to(half + core).start()
            merged_to(half + 2 + core).start()

    whole_top[...] = top

    @pl.when(early)
    def _():
        heard(far, half, max_sem.at[2]).wait_recv()
        most = whole_top[...]
        for d in range(half):
            most = jnp.maximum(most, far[d])
        whole_top[...] = most

    @pl.when(late)
    def _():
        merged_to(right).wait_recv()
        whole_top[...] = jnp.maximum(whole_top[...], merged[...])

    top = whole_top[...]
    over = 1.0 / top

    def place(owner, k):
        start, many = pieces[k]
        return whole.at[pl.ds(pl.multiple_of(owner * rows + start, 8), many), :]

    steps, count = chips // 2, len(pieces)
    ways = [(right, -2, right_recv), (left, 2, left_recv)]

    def when(condition, run):
        if condition is True:
            run()
        elif condition is not False:
            pl.when(condition)(run)

    def any_of(chosen):
        condition = False
        for c in chosen:
            condition = (chip == c) | condition
        return condition if chosen else False

    crossed = (6, 3)
    givers = (chips - 1, 1)
    odd, even = core == 1, core == 0

    def goes(way, step, k, shift):
        if step < steps - 1:
            return True
        if step == steps:
            return False
        to = 1 if way == 0 else -1
        takers = [c for c in range(chips) if (k in turned[c]) == (way == 0)]
        senders = [(c - shift * to) % chips for c in takers]
        return True if len(senders) == chips else any_of(senders)

    groups = [(0,), (3, 1, 5), (2, 6, 4)]
    comes = [[k for k in range(count) if any((k in t) == (way == 0) for t in turned)] for way in range(2)]

    def of_group(owner, g):
        start = pieces[groups[g][0]][0]
        many = sum(pieces[k][1] for k in groups[g])
        return whole.at[pl.ds(pl.multiple_of(owner * rows + start, 8), many), :]

    def group_onward(way, step, g):
        device, back, recv = ways[way]

        def run():
            ref = of_group(lax.rem(me + back * step + 2 * n, n), g)
            sent(ref, ref, device, send_sem.at[0], recv.at[step * len(groups) + g]).start()

        ahead_too = step == 0 and g == 0
        when(jnp.logical_not(to_left if way == 1 else to_right) if ahead_too else True, run)

    def last_sem(way, k):
        return ways[way][2].at[(steps - 1) * len(groups) + comes[way].index(k)]

    def onward(way, step, k):
        device, back, recv = ways[way]
        if k not in comes[way]:
            return

        def run():
            ref = place(lax.rem(me + back * step + 2 * n, n), k)
            sent(ref, ref, device, send_sem.at[0], last_sem(way, k)).start()

        condition = goes(way, step, k, 1)
        if step == steps - 1 and k == crossed[way]:
            condition = condition & jnp.logical_not((chip == givers[way]) & even)
        when(condition, run)

    def aside(owner, k, sem=0):
        ref = place(owner, k)
        sent(ref, ref, sibling, send_sem.at[0], side_sem.at[sem]).start()

    def handed(way):
        owner = lax.rem(2 * chip + (-2, 2)[way] * (steps - 1) + 2 * n, n)
        return owner, place(owner, crossed[way])

    def taken(way):
        owner = lax.rem(2 * chip + (-2, 2)[way] * steps + 2 * n, n)
        return owner, place(owner, crossed[way])

    def group_aside(owner, g):
        ref = of_group(owner, g)
        sent(ref, ref, sibling, send_sem.at[0], side_sem.at[0]).start()

    def scaled(rows_of, to):
        for t in range(tiles):
            at = pl.ds(128 * t, 128)
            to[:, at] = (rows_of[:, at] * over[t : t + 1, :]).astype(jnp.bfloat16)

    for g, group in enumerate(groups):
        for k in group:
            start, many = pieces[k]
            scaled(gained.at[pl.ds(start, many), :], place(me, k))
        group_onward(0, 0, g)
        group_onward(1, 0, g)
        group_aside(me, g)
    t = 0
    for out in (scale_query, scale_key, scale_value):
        for p in range(out.shape[0] // 128):
            out[pl.ds(128 * p, 128)] = top[t, :]
            t += 1

    for step in range(steps - 1):
        for g, group in enumerate(groups):
            for way, (device, back, recv) in enumerate(ways):
                owner = lax.rem(me + back * (step + 1) + 2 * n, n)
                ref = of_group(owner, g)
                sem = recv.at[step * len(groups) + g]
                arrived = sent(ref, ref, device, send_sem.at[0], sem)
                if step == 0 and g == 0:
                    came = from_left if way == 0 else from_right

                    @pl.when(came)
                    def _():
                        (right_rows if way == 0 else left_rows).wait_recv()
                        scaled(ahead.at[way], ref)

                    pl.when(jnp.logical_not(came))(arrived.wait_recv)
                else:
                    arrived.wait_recv()
                if step < steps - 2:
                    group_onward(way, step + 1, g)
                    group_aside(owner, g)
                    continue
                for k in group:
                    onward(way, step + 1, k)
                if crossed[way] not in group:
                    group_aside(owner, g)
                    continue
                hands = (chip == givers[way]) & even

                @pl.when(hands)
                def _():
                    for k in group:
                        aside(owner, k, int(k == crossed[way]))

                pl.when(jnp.logical_not(hands))(lambda: group_aside(owner, g))

                @pl.when((chip == givers[way]) & odd)
                def _():
                    _, ref = handed(way)
                    sent(ref, ref, sibling, send_sem.at[0], side_sem.at[1]).wait_recv()
                    sent(ref, ref, device, send_sem.at[0], side_sem.at[2 + way]).start()

    for k in (k for group in groups for k in group):
        for way, (device, back, recv) in enumerate(ways):
            if k not in comes[way]:
                continue
            owner = lax.rem(me + back * steps + 2 * n, n)
            ref = place(owner, k)
            arrived = sent(ref, ref, device, send_sem.at[0], last_sem(way, k))

            def run():
                arrived.wait_recv()
                aside(owner, k)

            condition = goes(way, steps - 1, k, 0)
            if k == crossed[way]:
                condition = condition & jnp.logical_not(lower & even)
            when(condition, run)
            if k == crossed[way]:

                @pl.when(lower & odd)
                def _():
                    owner, ref = taken(way)
                    sent(ref, ref, device, send_sem.at[0], side_sem.at[2 + way]).wait_recv()
                    aside(owner, k)

    more = [pieces[k][1] for k in crossed]
    got, gave = {}, {}

    by_right = [sum(pieces[k][1] for k in turned[c]) for c in range(chips)]
    for c in range(chips):
        total = (2 * chips - 1) * rows + by_right[(c + 1) % chips] - by_right[c - 1]
        total -= AHEAD * ((c < chips // 2 - 1) + (0 < c < chips // 2))
        for j in range(2):
            sign, shift = 2 * j - 1, 0
            if c == 0:
                shift = sum(more)
            if c in givers:
                shift += more[givers.index(c)]
            gave.setdefault(total + sign * shift, []).append((c, j))
            count = chips * rows
            if c == 0:
                count -= sign * sum(more)
            if c in givers and j == 1:
                count -= more[givers.index(c)]
            got.setdefault(count, []).append((c, j))

    def one_of(chosen):
        whole_chips = [c for c, j in chosen if j == 0 and (c, 1) in chosen]
        condition = any_of(whole_chips)
        for c, j in chosen:
            if c not in whole_chips:
                condition = ((chip == c) & (core == j)) | condition
        return condition

    for kind, totals in (("got", got), ("gave", gave)):
        for total, chosen in totals.items():

            @pl.when(one_of(chosen))
            def _():
                ref = whole.at[pl.ds(0, total), :]
                copy = sent(ref, ref, sibling, send_sem.at[0], side_sem.at[0])
                copy.wait_recv() if kind == "got" else copy.wait_send()

    @pl.when(early)
    def _():
        heard(maxima, half - 1, max_sem.at[1]).wait_send()
        pl.when(to_right)(right_rows.wait_send)
        pl.when(to_left)(left_rows.wait_send)

    @pl.when(late)
    def _():
        both = maxima.at[pl.ds(0, n - 1)]
        sent(both, both, right, max_sem.at[0], max_sem.at[1]).wait_send()

    @pl.when(lower | upper)
    def _():
        both = maxima.at[pl.ds(0, 2)]
        sent(both, both, right, max_sem.at[4], max_sem.at[3]).wait_send()


def stored(whole, one, two, three, query, key, value, scale_query, scale_key, scale_value, sems):
    length = whole.shape[0] // STORES
    at, copies = 0, []
    for out in (query, key, value):
        for p in range(STORES):
            part = pl.ds(p * length, length)
            copies.append((whole.at[part, pl.ds(at, out.shape[1])], out.at[part, :]))
        at += out.shape[1]
    copies += [(one, scale_query), (two, scale_key), (three, scale_value)]
    copies = [
        pltpu.make_async_copy(src, dst, sems.at[max(0, i - 3 * STORES + 1)])
        for i, (src, dst) in enumerate(copies)
    ]
    for copy in copies:
        copy.start()
    pltpu.make_async_copy(whole, whole, sems.at[0]).wait()
    for copy in copies[3 * STORES :]:
        copy.wait()


def shards(
    one_query, other_query, one_key, other_key, one_value, other_value, mix_share, norm_gain
):
    n = lax.axis_size("shard")
    rows, wide = one_query.shape
    narrow = one_key.shape[1]
    width = wide + 2 * narrow
    middle, small = rows // 2, 16
    moved = AHEAD // 2
    pieces = [
        (0, AHEAD),
        (middle + moved, middle - moved - small),
        (AHEAD, middle - 2 * moved - AHEAD),
        (middle, moved),
        (middle - moved, moved),
        (rows - small, small),
        (middle - 2 * moved, moved),
    ]
    chips = n // 2
    turned = [(0, 2, 4, 6)] * chips
    turned[0] = (0, 2, 6)
    turned[chips // 2 - 1] = (0, 2, 3, 4, 6)
    turned[chips // 2] = (0, 2, 6)
    turned[chips - 1] = (0, 2, 3, 4, 6)
    steps = n // 4
    full = [(rows, wide)] * 2 + [(rows, narrow)] * 4
    hbm = pl.BlockSpec(memory_space=pltpu.HBM)
    vmem = pl.BlockSpec(memory_space=pltpu.VMEM)
    scales = [((wide,), jnp.float32), ((narrow,), jnp.float32), ((narrow,), jnp.float32)]
    gathered = pl.pallas_call(
        functools.partial(kernel, n, pieces, turned),
        out_shape=[pltpu.VMEM((n * rows, width), jnp.bfloat16)]
        + [pltpu.VMEM(shape, dtype) for shape, dtype in scales],
        in_specs=[hbm] * 8,
        out_specs=[vmem] * 4,
        scratch_shapes=[
            tuple(pltpu.VMEM(shape, jnp.float32) for shape in full)
            + (pltpu.VMEM((rows,), jnp.float32),) * 2,
            pltpu.VMEM((rows, 128), jnp.float32),
            pltpu.VMEM((rows, 128), jnp.float32),
            pltpu.VMEM((rows, width), jnp.float32),
            pltpu.VMEM((n, width // 128, 128), jnp.float32),
            pltpu.VMEM((n // 2, width // 128, 128), jnp.float32),
            pltpu.VMEM((width // 128, 128), jnp.float32),
            pltpu.VMEM((width // 128, 128), jnp.float32),
            pltpu.VMEM((2, AHEAD, width), jnp.float32),
            pltpu.SemaphoreType.DMA((8,)),
            pltpu.SemaphoreType.DMA((5,)),
            pltpu.SemaphoreType.DMA((4,)),
            pltpu.SemaphoreType.REGULAR,
            pltpu.SemaphoreType.DMA((1,)),
            pltpu.SemaphoreType.DMA((4,)),
            pltpu.SemaphoreType.DMA((3 * steps + 2,)),
            pltpu.SemaphoreType.DMA((3 * steps + 1,)),
        ],
        compiler_params=pltpu.CompilerParams(
            collective_id=0, has_side_effects=True, vmem_limit_bytes=24 * 2**20
        ),
    )(
        *(
            pltpu.with_memory_space_constraint(x, pltpu.HBM)
            for x in (
                one_query,
                other_query,
                one_key,
                other_key,
                one_value,
                other_value,
                mix_share,
                norm_gain,
            )
        )
    )
    outs = [((n * rows, wide), jnp.bfloat16)] + [((n * rows, narrow), jnp.bfloat16)] * 2 + scales
    return pl.pallas_call(
        stored,
        out_shape=[pltpu.HBM(shape, dtype) for shape, dtype in outs],
        in_specs=[vmem] * 4,
        out_specs=[hbm] * 6,
        scratch_shapes=[pltpu.SemaphoreType.DMA((4,))],
        compiler_params=pltpu.CompilerParams(vmem_limit_bytes=2**20),
    )(*gathered)


def solution(mesh):
    placed = (
        P(("job", "shard"), "cols"),
        P(("job", "shard"), "cols"),
        P(("job", "shard"), "cols"),
        P(("job", "shard"), "cols"),
        P(("job", "shard"), "cols"),
        P(("job", "shard"), "cols"),
        P(("job", "shard")),
        P(("job", "shard")),
    )
    return jax.shard_map(
        shards,
        mesh=mesh,
        in_specs=placed,
        out_specs=(
            P("job", "cols"),
            P("job", "cols"),
            P("job", "cols"),
            P(("job", "cols")),
            P(("job", "cols")),
            P(("job", "cols")),
        ),
        check_vma=False,
    )
```

```python
import functools

import jax
import jax.numpy as jnp
from jax import lax
from jax.experimental import pallas as pl
from jax.experimental.pallas import tpu as pltpu
from jax.sharding import PartitionSpec as P

MESH = pl.DeviceIdType.MESH
STORES = 2
AHEAD = 48


def kernel(
    n,
    pieces,
    turned,
    one_query,
    other_query,
    one_key,
    other_key,
    one_value,
    other_value,
    mix_share,
    norm_gain,
    whole,
    scale_query,
    scale_key,
    scale_value,
    ins,
    mix_a,
    mix_b,
    gained,
    maxima,
    far,
    merged,
    whole_top,
    ahead,
    load_sem,
    max_sem,
    ahead_sem,
    near_sem,
    send_sem,
    side_sem,
    right_recv,
    left_recv,
):
    one_q, other_q, one_k, other_k, one_v, other_v, share, gain = ins
    rows, wide = one_query.shape
    narrow = one_key.shape[1]
    chips, tiles = n // 2, (wide + 2 * narrow) // 128
    me = lax.axis_index("shard")
    core = lax.rem(me, 2)
    sibling = me + 1 - 2 * core
    right, left = lax.rem(me + 2, n), lax.rem(me + n - 2, n)

    chip, half = me // 2, n // 2
    early = chip < chips // 2
    late = jnp.logical_not(early)
    base = half * (me // half)
    barrier = pltpu.get_barrier_semaphore()

    def greet(device):
        pl.semaphore_signal(barrier, inc=1, device_id={"shard": device}, device_id_type=MESH)

    for d in range(1, half):
        greet(base + lax.rem(me + d, half))

    @pl.when(early)
    def _():
        for d in range(half):
            greet(half + d)

    loads = [
        pltpu.make_async_copy(src, dst, load_sem.at[i])
        for i, (src, dst) in enumerate(
            [
                (mix_share, share),
                (norm_gain, gain),
                (one_key, one_k),
                (other_key, other_k),
                (one_value, one_v),
                (other_value, other_v),
                (one_query, one_q),
                (other_query, other_q),
            ]
        )
    ]
    for load in loads:
        load.start()

    loads[0].wait()
    loads[1].wait()
    for t in range(rows // 128):
        at = pl.ds(128 * t, 128)
        m = jnp.broadcast_to(share[at].reshape(1, 128), (128, 128)).T
        g = jnp.broadcast_to(gain[at].reshape(1, 128), (128, 128)).T
        mix_a[at, :] = m * g
        mix_b[at, :] = (1.0 - m) * g

    def mixed(one, other, first, columns):
        for t in range(columns // 128):
            at, to = pl.ds(128 * t, 128), pl.ds(first + 128 * t, 128)
            x = mix_a[...] * one[:, at] + mix_b[...] * other[:, at]
            gained[:, to] = x
            maxima[0, pl.ds(first // 128 + t, 1), :] = jnp.max(jnp.abs(x), axis=0, keepdims=True)

    loads[2].wait()
    loads[3].wait()
    mixed(one_k, other_k, wide, narrow)
    loads[4].wait()
    loads[5].wait()
    mixed(one_v, other_v, wide + narrow, narrow)
    loads[6].wait()
    loads[7].wait()
    mixed(one_q, other_q, 0, wide)

    def sent(src, dst, device, send, recv):
        return pltpu.make_async_remote_copy(
            src_ref=src,
            dst_ref=dst,
            send_sem=send,
            recv_sem=recv,
            device_id={"shard": device},
            device_id_type=MESH,
        )

    lower, upper = chip == 0, chip == chips // 2 - 1
    to_right, to_left = chip < chips // 2 - 1, early & (chip > 0)
    from_left, from_right = to_left, to_right
    mine = maxima.at[0]

    def within(d):
        sent(
            mine, maxima.at[d], base + lax.rem(me + d, half), max_sem.at[0], max_sem.at[1]
        ).start()

    def heard(ref, count, recv):
        some = ref.at[pl.ds(0, count)]
        return sent(some, some, right, max_sem.at[0], recv)

    def merged_to(device):
        return sent(merged, merged, device, max_sem.at[4], max_sem.at[3])

    early_rows = gained.at[pl.ds(0, AHEAD), :]
    right_rows = sent(early_rows, ahead.at[0], right, ahead_sem.at[0], ahead_sem.at[2])
    left_rows = sent(early_rows, ahead.at[1], left, ahead_sem.at[1], ahead_sem.at[3])

    @pl.when(early)
    def _():
        pl.semaphore_wait(barrier, half - 1)
        for d in range(1, half):
            within(d)
        pl.when(to_right)(right_rows.start)
        pl.when(to_left)(left_rows.start)

    @pl.when(late)
    def _():
        pl.semaphore_wait(barrier, n - 1)
        close = core + (half - 2) * (1 - chip // (chips * 3 // 4))
        pl.semaphore_signal(near_sem, inc=1, device_id={"shard": close}, device_id_type=MESH)
        for d in sorted(range(half), key=lambda d: -min(d + 1, half - d)):
            peer = lax.rem(me + half // 2 + 1 + d, half)
            sent(mine, far.at[me - half], peer, max_sem.at[0], max_sem.at[2]).start()
        for d in range(1, half):
            within(d)

    heard(maxima, half - 1, max_sem.at[1]).wait_recv()
    top = maxima[0]
    for d in range(1, half):
        top = jnp.maximum(top, maxima[d])

    @pl.when(lower | upper)
    def _():
        merged[...] = top
        pl.semaphore_wait(near_sem, 2)

        @pl.when(lower)
        def _():
            merged_to(n - 2 + core).start()
            merged_to(n - 4 + core).start()

        @pl.when(upper)
        def _():
            merged_to(half + core).start()
            merged_to(half + 2 + core).start()

    whole_top[...] = top

    @pl.when(early)
    def _():
        heard(far, half, max_sem.at[2]).wait_recv()
        most = whole_top[...]
        for d in range(half):
            most = jnp.maximum(most, far[d])
        whole_top[...] = most

    @pl.when(late)
    def _():
        merged_to(right).wait_recv()
        whole_top[...] = jnp.maximum(whole_top[...], merged[...])

    top = whole_top[...]
    over = 1.0 / top

    def place(owner, k):
        start, many = pieces[k]
        return whole.at[pl.ds(pl.multiple_of(owner * rows + start, 8), many), :]

    steps, count = chips // 2, len(pieces)
    ways = [(right, -2, right_recv), (left, 2, left_recv)]

    def when(condition, run):
        if condition is True:
            run()
        elif condition is not False:
            pl.when(condition)(run)

    def any_of(chosen):
        condition = False
        for c in chosen:
            condition = (chip == c) | condition
        return condition if chosen else False

    crossed = (6, 3)
    givers = (chips - 1, 1)
    odd, even = core == 1, core == 0

    def goes(way, step, k, shift):
        if step < steps - 1:
            return True
        if step == steps:
            return False
        to = 1 if way == 0 else -1
        takers = [c for c in range(chips) if (k in turned[c]) == (way == 0)]
        senders = [(c - shift * to) % chips for c in takers]
        return True if len(senders) == chips else any_of(senders)

    groups = [(0,), (3, 1, 5), (2, 6, 4)]
    comes = [[k for k in range(count) if any((k in t) == (way == 0) for t in turned)] for way in range(2)]

    def of_group(owner, g):
        start = pieces[groups[g][0]][0]
        many = sum(pieces[k][1] for k in groups[g])
        return whole.at[pl.ds(pl.multiple_of(owner * rows + start, 8), many), :]

    def group_onward(way, step, g):
        device, back, recv = ways[way]

        def run():
            ref = of_group(lax.rem(me + back * step + 2 * n, n), g)
            sent(ref, ref, device, send_sem.at[0], recv.at[step * len(groups) + g]).start()

        ahead_too = step == 0 and g == 0
        when(jnp.logical_not(to_left if way == 1 else to_right) if ahead_too else True, run)

    def last_sem(way, k):
        return ways[way][2].at[(steps - 1) * len(groups) + comes[way].index(k)]

    def onward(way, step, k):
        device, back, recv = ways[way]
        if k not in comes[way]:
            return

        def run():
            ref = place(lax.rem(me + back * step + 2 * n, n), k)
            sent(ref, ref, device, send_sem.at[0], last_sem(way, k)).start()

        condition = goes(way, step, k, 1)
        if step == steps - 1 and k == crossed[way]:
            condition = condition & jnp.logical_not((chip == givers[way]) & even)
        when(condition, run)

    def aside(owner, k, sem=0):
        ref = place(owner, k)
        sent(ref, ref, sibling, send_sem.at[0], side_sem.at[sem]).start()

    def handed(way):
        owner = lax.rem(2 * chip + (-2, 2)[way] * (steps - 1) + 2 * n, n)
        return owner, place(owner, crossed[way])

    def taken(way):
        owner = lax.rem(2 * chip + (-2, 2)[way] * steps + 2 * n, n)
        return owner, place(owner, crossed[way])

    def group_aside(owner, g):
        ref = of_group(owner, g)
        sent(ref, ref, sibling, send_sem.at[0], side_sem.at[0]).start()

    def scaled(rows_of, to):
        for t in range(tiles):
            at = pl.ds(128 * t, 128)
            to[:, at] = (rows_of[:, at] * over[t : t + 1, :]).astype(jnp.bfloat16)

    for g, group in enumerate(groups):
        for k in group:
            start, many = pieces[k]
            scaled(gained.at[pl.ds(start, many), :], place(me, k))
        group_onward(0, 0, g)
        group_onward(1, 0, g)
        group_aside(me, g)
    t = 0
    for out in (scale_query, scale_key, scale_value):
        for p in range(out.shape[0] // 128):
            out[pl.ds(128 * p, 128)] = top[t, :]
            t += 1

    for step in range(steps - 1):
        for g, group in enumerate(groups):
            for way, (device, back, recv) in enumerate(ways):
                owner = lax.rem(me + back * (step + 1) + 2 * n, n)
                ref = of_group(owner, g)
                sem = recv.at[step * len(groups) + g]
                arrived = sent(ref, ref, device, send_sem.at[0], sem)
                if step == 0 and g == 0:
                    came = from_left if way == 0 else from_right

                    @pl.when(came)
                    def _():
                        (right_rows if way == 0 else left_rows).wait_recv()
                        scaled(ahead.at[way], ref)

                    pl.when(jnp.logical_not(came))(arrived.wait_recv)
                else:
                    arrived.wait_recv()
                if step < steps - 2:
                    group_onward(way, step + 1, g)
                    group_aside(owner, g)
                    continue
                for k in group:
                    onward(way, step + 1, k)
                if crossed[way] not in group:
                    group_aside(owner, g)
                    continue
                hands = (chip == givers[way]) & even

                @pl.when(hands)
                def _():
                    for k in group:
                        aside(owner, k, int(k == crossed[way]))

                pl.when(jnp.logical_not(hands))(lambda: group_aside(owner, g))

                @pl.when((chip == givers[way]) & odd)
                def _():
                    _, ref = handed(way)
                    sent(ref, ref, sibling, send_sem.at[0], side_sem.at[1]).wait_recv()
                    sent(ref, ref, device, send_sem.at[0], side_sem.at[2 + way]).start()

    for k in (k for group in groups for k in group):
        for way, (device, back, recv) in enumerate(ways):
            if k not in comes[way]:
                continue
            owner = lax.rem(me + back * steps + 2 * n, n)
            ref = place(owner, k)
            arrived = sent(ref, ref, device, send_sem.at[0], last_sem(way, k))

            def run():
                arrived.wait_recv()
                aside(owner, k)

            condition = goes(way, steps - 1, k, 0)
            if k == crossed[way]:
                condition = condition & jnp.logical_not(lower & even)
            when(condition, run)
            if k == crossed[way]:

                @pl.when(lower & odd)
                def _():
                    owner, ref = taken(way)
                    sent(ref, ref, device, send_sem.at[0], side_sem.at[2 + way]).wait_recv()
                    aside(owner, k)

    more = [pieces[k][1] for k in crossed]
    got, gave = {}, {}

    by_right = [sum(pieces[k][1] for k in turned[c]) for c in range(chips)]
    for c in range(chips):
        total = (2 * chips - 1) * rows + by_right[(c + 1) % chips] - by_right[c - 1]
        total -= AHEAD * ((c < chips // 2 - 1) + (0 < c < chips // 2))
        for j in range(2):
            sign, shift = 2 * j - 1, 0
            if c == 0:
                shift = sum(more)
            if c in givers:
                shift += more[givers.index(c)]
            gave.setdefault(total + sign * shift, []).append((c, j))
            count = chips * rows
            if c == 0:
                count -= sign * sum(more)
            if c in givers and j == 1:
                count -= more[givers.index(c)]
            got.setdefault(count, []).append((c, j))

    def one_of(chosen):
        whole_chips = [c for c, j in chosen if j == 0 and (c, 1) in chosen]
        condition = any_of(whole_chips)
        for c, j in chosen:
            if c not in whole_chips:
                condition = ((chip == c) & (core == j)) | condition
        return condition

    for kind, totals in (("got", got), ("gave", gave)):
        for total, chosen in totals.items():

            @pl.when(one_of(chosen))
            def _():
                ref = whole.at[pl.ds(0, total), :]
                copy = sent(ref, ref, sibling, send_sem.at[0], side_sem.at[0])
                copy.wait_recv() if kind == "got" else copy.wait_send()

    @pl.when(early)
    def _():
        heard(maxima, half - 1, max_sem.at[1]).wait_send()
        pl.when(to_right)(right_rows.wait_send)
        pl.when(to_left)(left_rows.wait_send)

    @pl.when(late)
    def _():
        both = maxima.at[pl.ds(0, n - 1)]
        sent(both, both, right, max_sem.at[0], max_sem.at[1]).wait_send()

    @pl.when(lower | upper)
    def _():
        both = maxima.at[pl.ds(0, 2)]
        sent(both, both, right, max_sem.at[4], max_sem.at[3]).wait_send()


def stored(whole, one, two, three, query, key, value, scale_query, scale_key, scale_value, sems):
    length = whole.shape[0] // STORES
    at, copies = 0, []
    for out in (query, key, value):
        for p in range(STORES):
            part = pl.ds(p * length, length)
            copies.append((whole.at[part, pl.ds(at, out.shape[1])], out.at[part, :]))
        at += out.shape[1]
    copies += [(one, scale_query), (two, scale_key), (three, scale_value)]
    copies = [
        pltpu.make_async_copy(src, dst, sems.at[max(0, i - 3 * STORES + 1)])
        for i, (src, dst) in enumerate(copies)
    ]
    for copy in copies:
        copy.start()
    pltpu.make_async_copy(whole, whole, sems.at[0]).wait()
    for copy in copies[3 * STORES :]:
        copy.wait()


def shards(
    one_query, other_query, one_key, other_key, one_value, other_value, mix_share, norm_gain
):
    n = lax.axis_size("shard")
    rows, wide = one_query.shape
    narrow = one_key.shape[1]
    width = wide + 2 * narrow
    middle, small = rows // 2, 16
    moved = 32
    pieces = [
        (0, AHEAD),
        (middle + moved, middle - moved - small),
        (AHEAD, middle - 2 * moved - AHEAD),
        (middle, moved),
        (middle - moved, moved),
        (rows - small, small),
        (middle - 2 * moved, moved),
    ]
    chips = n // 2
    turned = [(0, 2, 4, 6)] * chips
    turned[0] = (0, 2, 6)
    turned[chips // 2 - 1] = (0, 2, 3, 4, 6)
    turned[chips // 2] = (0, 2, 6)
    turned[chips - 1] = (0, 2, 3, 4, 6)
    steps = n // 4
    full = [(rows, wide)] * 2 + [(rows, narrow)] * 4
    hbm = pl.BlockSpec(memory_space=pltpu.HBM)
    vmem = pl.BlockSpec(memory_space=pltpu.VMEM)
    scales = [((wide,), jnp.float32), ((narrow,), jnp.float32), ((narrow,), jnp.float32)]
    gathered = pl.pallas_call(
        functools.partial(kernel, n, pieces, turned),
        out_shape=[pltpu.VMEM((n * rows, width), jnp.bfloat16)]
        + [pltpu.VMEM(shape, dtype) for shape, dtype in scales],
        in_specs=[hbm] * 8,
        out_specs=[vmem] * 4,
        scratch_shapes=[
            tuple(pltpu.VMEM(shape, jnp.float32) for shape in full)
            + (pltpu.VMEM((rows,), jnp.float32),) * 2,
            pltpu.VMEM((rows, 128), jnp.float32),
            pltpu.VMEM((rows, 128), jnp.float32),
            pltpu.VMEM((rows, width), jnp.float32),
            pltpu.VMEM((n, width // 128, 128), jnp.float32),
            pltpu.VMEM((n // 2, width // 128, 128), jnp.float32),
            pltpu.VMEM((width // 128, 128), jnp.float32),
            pltpu.VMEM((width // 128, 128), jnp.float32),
            pltpu.VMEM((2, AHEAD, width), jnp.float32),
            pltpu.SemaphoreType.DMA((8,)),
            pltpu.SemaphoreType.DMA((5,)),
            pltpu.SemaphoreType.DMA((4,)),
            pltpu.SemaphoreType.REGULAR,
            pltpu.SemaphoreType.DMA((1,)),
            pltpu.SemaphoreType.DMA((4,)),
            pltpu.SemaphoreType.DMA((3 * steps + 2,)),
            pltpu.SemaphoreType.DMA((3 * steps + 1,)),
        ],
        compiler_params=pltpu.CompilerParams(
            collective_id=0, has_side_effects=True, vmem_limit_bytes=24 * 2**20
        ),
    )(
        *(
            pltpu.with_memory_space_constraint(x, pltpu.HBM)
            for x in (
                one_query,
                other_query,
                one_key,
                other_key,
                one_value,
                other_value,
                mix_share,
                norm_gain,
            )
        )
    )
    outs = [((n * rows, wide), jnp.bfloat16)] + [((n * rows, narrow), jnp.bfloat16)] * 2 + scales
    return pl.pallas_call(
        stored,
        out_shape=[pltpu.HBM(shape, dtype) for shape, dtype in outs],
        in_specs=[vmem] * 4,
        out_specs=[hbm] * 6,
        scratch_shapes=[pltpu.SemaphoreType.DMA((4,))],
        compiler_params=pltpu.CompilerParams(vmem_limit_bytes=2**20),
    )(*gathered)


def solution(mesh):
    placed = (
        P(("job", "shard"), "cols"),
        P(("job", "shard"), "cols"),
        P(("job", "shard"), "cols"),
        P(("job", "shard"), "cols"),
        P(("job", "shard"), "cols"),
        P(("job", "shard"), "cols"),
        P(("job", "shard")),
        P(("job", "shard")),
    )
    return jax.shard_map(
        shards,
        mesh=mesh,
        in_specs=placed,
        out_specs=(
            P("job", "cols"),
            P("job", "cols"),
            P("job", "cols"),
            P(("job", "cols")),
            P(("job", "cols")),
            P(("job", "cols")),
        ),
        check_vma=False,
    )
```

```python
import functools

import jax
import jax.numpy as jnp
from jax import lax
from jax.experimental import pallas as pl
from jax.experimental.pallas import tpu as pltpu
from jax.sharding import PartitionSpec as P

MESH = pl.DeviceIdType.MESH
STORES = 2
AHEAD = 40


def kernel(
    n,
    pieces,
    turned,
    one_query,
    other_query,
    one_key,
    other_key,
    one_value,
    other_value,
    mix_share,
    norm_gain,
    whole,
    scale_query,
    scale_key,
    scale_value,
    ins,
    mix_a,
    mix_b,
    gained,
    maxima,
    far,
    merged,
    whole_top,
    ahead,
    load_sem,
    max_sem,
    ahead_sem,
    near_sem,
    send_sem,
    side_sem,
    right_recv,
    left_recv,
):
    one_q, other_q, one_k, other_k, one_v, other_v, share, gain = ins
    rows, wide = one_query.shape
    narrow = one_key.shape[1]
    chips, tiles = n // 2, (wide + 2 * narrow) // 128
    me = lax.axis_index("shard")
    core = lax.rem(me, 2)
    sibling = me + 1 - 2 * core
    right, left = lax.rem(me + 2, n), lax.rem(me + n - 2, n)

    chip, half = me // 2, n // 2
    early = chip < chips // 2
    late = jnp.logical_not(early)
    base = half * (me // half)
    barrier = pltpu.get_barrier_semaphore()

    def greet(device):
        pl.semaphore_signal(barrier, inc=1, device_id={"shard": device}, device_id_type=MESH)

    for d in range(1, half):
        greet(base + lax.rem(me + d, half))

    @pl.when(early)
    def _():
        for d in range(half):
            greet(half + d)

    loads = [
        pltpu.make_async_copy(src, dst, load_sem.at[i])
        for i, (src, dst) in enumerate(
            [
                (mix_share, share),
                (norm_gain, gain),
                (one_key, one_k),
                (other_key, other_k),
                (one_value, one_v),
                (other_value, other_v),
                (one_query, one_q),
                (other_query, other_q),
            ]
        )
    ]
    for load in loads:
        load.start()

    loads[0].wait()
    loads[1].wait()
    for t in range(rows // 128):
        at = pl.ds(128 * t, 128)
        m = jnp.broadcast_to(share[at].reshape(1, 128), (128, 128)).T
        g = jnp.broadcast_to(gain[at].reshape(1, 128), (128, 128)).T
        mix_a[at, :] = m * g
        mix_b[at, :] = (1.0 - m) * g

    def mixed(one, other, first, columns):
        for t in range(columns // 128):
            at, to = pl.ds(128 * t, 128), pl.ds(first + 128 * t, 128)
            x = mix_a[...] * one[:, at] + mix_b[...] * other[:, at]
            gained[:, to] = x
            maxima[0, pl.ds(first // 128 + t, 1), :] = jnp.max(jnp.abs(x), axis=0, keepdims=True)

    loads[2].wait()
    loads[3].wait()
    mixed(one_k, other_k, wide, narrow)
    loads[4].wait()
    loads[5].wait()
    mixed(one_v, other_v, wide + narrow, narrow)
    loads[6].wait()
    loads[7].wait()
    mixed(one_q, other_q, 0, wide)

    def sent(src, dst, device, send, recv):
        return pltpu.make_async_remote_copy(
            src_ref=src,
            dst_ref=dst,
            send_sem=send,
            recv_sem=recv,
            device_id={"shard": device},
            device_id_type=MESH,
        )

    lower, upper = chip == 0, chip == chips // 2 - 1
    to_right, to_left = chip < chips // 2 - 1, early & (chip > 0)
    from_left, from_right = to_left, to_right
    mine = maxima.at[0]

    def within(d):
        sent(
            mine, maxima.at[d], base + lax.rem(me + d, half), max_sem.at[0], max_sem.at[1]
        ).start()

    def heard(ref, count, recv):
        some = ref.at[pl.ds(0, count)]
        return sent(some, some, right, max_sem.at[0], recv)

    def merged_to(device):
        return sent(merged, merged, device, max_sem.at[4], max_sem.at[3])

    early_rows = gained.at[pl.ds(0, AHEAD), :]
    right_rows = sent(early_rows, ahead.at[0], right, ahead_sem.at[0], ahead_sem.at[2])
    left_rows = sent(early_rows, ahead.at[1], left, ahead_sem.at[1], ahead_sem.at[3])

    @pl.when(early)
    def _():
        pl.semaphore_wait(barrier, half - 1)
        for d in range(1, half):
            within(d)
        pl.when(to_right)(right_rows.start)
        pl.when(to_left)(left_rows.start)

    @pl.when(late)
    def _():
        pl.semaphore_wait(barrier, n - 1)
        close = core + (half - 2) * (1 - chip // (chips * 3 // 4))
        pl.semaphore_signal(near_sem, inc=1, device_id={"shard": close}, device_id_type=MESH)
        for d in sorted(range(half), key=lambda d: -min(d + 1, half - d)):
            peer = lax.rem(me + half // 2 + 1 + d, half)
            sent(mine, far.at[me - half], peer, max_sem.at[0], max_sem.at[2]).start()
        for d in range(1, half):
            within(d)

    heard(maxima, half - 1, max_sem.at[1]).wait_recv()
    top = maxima[0]
    for d in range(1, half):
        top = jnp.maximum(top, maxima[d])

    @pl.when(lower | upper)
    def _():
        merged[...] = top
        pl.semaphore_wait(near_sem, 2)

        @pl.when(lower)
        def _():
            merged_to(n - 2 + core).start()
            merged_to(n - 4 + core).start()

        @pl.when(upper)
        def _():
            merged_to(half + core).start()
            merged_to(half + 2 + core).start()

    whole_top[...] = top

    @pl.when(early)
    def _():
        heard(far, half, max_sem.at[2]).wait_recv()
        most = whole_top[...]
        for d in range(half):
            most = jnp.maximum(most, far[d])
        whole_top[...] = most

    @pl.when(late)
    def _():
        merged_to(right).wait_recv()
        whole_top[...] = jnp.maximum(whole_top[...], merged[...])

    top = whole_top[...]
    over = 1.0 / top

    def place(owner, k):
        start, many = pieces[k]
        return whole.at[pl.ds(pl.multiple_of(owner * rows + start, 8), many), :]

    steps, count = chips // 2, len(pieces)
    ways = [(right, -2, right_recv), (left, 2, left_recv)]

    def when(condition, run):
        if condition is True:
            run()
        elif condition is not False:
            pl.when(condition)(run)

    def any_of(chosen):
        condition = False
        for c in chosen:
            condition = (chip == c) | condition
        return condition if chosen else False

    crossed = (6, 3)
    givers = (chips - 1, 1)
    odd, even = core == 1, core == 0

    def goes(way, step, k, shift):
        if step < steps - 1:
            return True
        if step == steps:
            return False
        to = 1 if way == 0 else -1
        takers = [c for c in range(chips) if (k in turned[c]) == (way == 0)]
        senders = [(c - shift * to) % chips for c in takers]
        return True if len(senders) == chips else any_of(senders)

    groups = [(0,), (3, 1, 5), (2, 6, 4)]
    comes = [[k for k in range(count) if any((k in t) == (way == 0) for t in turned)] for way in range(2)]

    def of_group(owner, g):
        start = pieces[groups[g][0]][0]
        many = sum(pieces[k][1] for k in groups[g])
        return whole.at[pl.ds(pl.multiple_of(owner * rows + start, 8), many), :]

    def group_onward(way, step, g):
        device, back, recv = ways[way]

        def run():
            ref = of_group(lax.rem(me + back * step + 2 * n, n), g)
            sent(ref, ref, device, send_sem.at[0], recv.at[step * len(groups) + g]).start()

        ahead_too = step == 0 and g == 0
        when(jnp.logical_not(to_left if way == 1 else to_right) if ahead_too else True, run)

    def last_sem(way, k):
        return ways[way][2].at[(steps - 1) * len(groups) + comes[way].index(k)]

    def onward(way, step, k):
        device, back, recv = ways[way]
        if k not in comes[way]:
            return

        def run():
            ref = place(lax.rem(me + back * step + 2 * n, n), k)
            sent(ref, ref, device, send_sem.at[0], last_sem(way, k)).start()

        condition = goes(way, step, k, 1)
        if step == steps - 1 and k == crossed[way]:
            condition = condition & jnp.logical_not((chip == givers[way]) & even)
        when(condition, run)

    def aside(owner, k, sem=0):
        ref = place(owner, k)
        sent(ref, ref, sibling, send_sem.at[0], side_sem.at[sem]).start()

    def handed(way):
        owner = lax.rem(2 * chip + (-2, 2)[way] * (steps - 1) + 2 * n, n)
        return owner, place(owner, crossed[way])

    def taken(way):
        owner = lax.rem(2 * chip + (-2, 2)[way] * steps + 2 * n, n)
        return owner, place(owner, crossed[way])

    def group_aside(owner, g):
        ref = of_group(owner, g)
        sent(ref, ref, sibling, send_sem.at[0], side_sem.at[0]).start()

    def scaled(rows_of, to):
        for t in range(tiles):
            at = pl.ds(128 * t, 128)
            to[:, at] = (rows_of[:, at] * over[t : t + 1, :]).astype(jnp.bfloat16)

    for g, group in enumerate(groups):
        for k in group:
            start, many = pieces[k]
            scaled(gained.at[pl.ds(start, many), :], place(me, k))
        group_onward(0, 0, g)
        group_onward(1, 0, g)
        group_aside(me, g)
    t = 0
    for out in (scale_query, scale_key, scale_value):
        for p in range(out.shape[0] // 128):
            out[pl.ds(128 * p, 128)] = top[t, :]
            t += 1

    for step in range(steps - 1):
        for g, group in enumerate(groups):
            for way, (device, back, recv) in enumerate(ways):
                owner = lax.rem(me + back * (step + 1) + 2 * n, n)
                ref = of_group(owner, g)
                sem = recv.at[step * len(groups) + g]
                arrived = sent(ref, ref, device, send_sem.at[0], sem)
                if step == 0 and g == 0:
                    came = from_left if way == 0 else from_right

                    @pl.when(came)
                    def _():
                        (right_rows if way == 0 else left_rows).wait_recv()
                        scaled(ahead.at[way], ref)

                    pl.when(jnp.logical_not(came))(arrived.wait_recv)
                else:
                    arrived.wait_recv()
                if step < steps - 2:
                    group_onward(way, step + 1, g)
                    group_aside(owner, g)
                    continue
                for k in group:
                    onward(way, step + 1, k)
                if crossed[way] not in group:
                    group_aside(owner, g)
                    continue
                hands = (chip == givers[way]) & even

                @pl.when(hands)
                def _():
                    for k in group:
                        aside(owner, k, int(k == crossed[way]))

                pl.when(jnp.logical_not(hands))(lambda: group_aside(owner, g))

                @pl.when((chip == givers[way]) & odd)
                def _():
                    _, ref = handed(way)
                    sent(ref, ref, sibling, send_sem.at[0], side_sem.at[1]).wait_recv()
                    sent(ref, ref, device, send_sem.at[0], side_sem.at[2 + way]).start()

    for k in (k for group in groups for k in group):
        for way, (device, back, recv) in enumerate(ways):
            if k not in comes[way]:
                continue
            owner = lax.rem(me + back * steps + 2 * n, n)
            ref = place(owner, k)
            arrived = sent(ref, ref, device, send_sem.at[0], last_sem(way, k))

            def run():
                arrived.wait_recv()
                aside(owner, k)

            condition = goes(way, steps - 1, k, 0)
            if k == crossed[way]:
                condition = condition & jnp.logical_not(lower & even)
            when(condition, run)
            if k == crossed[way]:

                @pl.when(lower & odd)
                def _():
                    owner, ref = taken(way)
                    sent(ref, ref, device, send_sem.at[0], side_sem.at[2 + way]).wait_recv()
                    aside(owner, k)

    more = [pieces[k][1] for k in crossed]
    got, gave = {}, {}

    by_right = [sum(pieces[k][1] for k in turned[c]) for c in range(chips)]
    for c in range(chips):
        total = (2 * chips - 1) * rows + by_right[(c + 1) % chips] - by_right[c - 1]
        total -= AHEAD * ((c < chips // 2 - 1) + (0 < c < chips // 2))
        for j in range(2):
            sign, shift = 2 * j - 1, 0
            if c == 0:
                shift = sum(more)
            if c in givers:
                shift += more[givers.index(c)]
            gave.setdefault(total + sign * shift, []).append((c, j))
            count = chips * rows
            if c == 0:
                count -= sign * sum(more)
            if c in givers and j == 1:
                count -= more[givers.index(c)]
            got.setdefault(count, []).append((c, j))

    def one_of(chosen):
        whole_chips = [c for c, j in chosen if j == 0 and (c, 1) in chosen]
        condition = any_of(whole_chips)
        for c, j in chosen:
            if c not in whole_chips:
                condition = ((chip == c) & (core == j)) | condition
        return condition

    for kind, totals in (("got", got), ("gave", gave)):
        for total, chosen in totals.items():

            @pl.when(one_of(chosen))
            def _():
                ref = whole.at[pl.ds(0, total), :]
                copy = sent(ref, ref, sibling, send_sem.at[0], side_sem.at[0])
                copy.wait_recv() if kind == "got" else copy.wait_send()

    @pl.when(early)
    def _():
        heard(maxima, half - 1, max_sem.at[1]).wait_send()
        pl.when(to_right)(right_rows.wait_send)
        pl.when(to_left)(left_rows.wait_send)

    @pl.when(late)
    def _():
        both = maxima.at[pl.ds(0, n - 1)]
        sent(both, both, right, max_sem.at[0], max_sem.at[1]).wait_send()

    @pl.when(lower | upper)
    def _():
        both = maxima.at[pl.ds(0, 2)]
        sent(both, both, right, max_sem.at[4], max_sem.at[3]).wait_send()


def stored(whole, one, two, three, query, key, value, scale_query, scale_key, scale_value, sems):
    length = whole.shape[0] // STORES
    at, copies = 0, []
    for out in (query, key, value):
        for p in range(STORES):
            part = pl.ds(p * length, length)
            copies.append((whole.at[part, pl.ds(at, out.shape[1])], out.at[part, :]))
        at += out.shape[1]
    copies += [(one, scale_query), (two, scale_key), (three, scale_value)]
    copies = [
        pltpu.make_async_copy(src, dst, sems.at[max(0, i - 3 * STORES + 1)])
        for i, (src, dst) in enumerate(copies)
    ]
    for copy in copies:
        copy.start()
    pltpu.make_async_copy(whole, whole, sems.at[0]).wait()
    for copy in copies[3 * STORES :]:
        copy.wait()


def shards(
    one_query, other_query, one_key, other_key, one_value, other_value, mix_share, norm_gain
):
    n = lax.axis_size("shard")
    rows, wide = one_query.shape
    narrow = one_key.shape[1]
    width = wide + 2 * narrow
    middle, small = rows // 2, 16
    moved = 40
    pieces = [
        (0, AHEAD),
        (middle + moved, middle - moved - small),
        (AHEAD, middle - 2 * moved - AHEAD),
        (middle, moved),
        (middle - moved, moved),
        (rows - small, small),
        (middle - 2 * moved, moved),
    ]
    chips = n // 2
    turned = [(0, 2, 4, 6)] * chips
    turned[0] = (0, 2, 6)
    turned[chips // 2 - 1] = (0, 2, 3, 4, 6)
    turned[chips // 2] = (0, 2, 6)
    turned[chips - 1] = (0, 2, 3, 4, 6)
    steps = n // 4
    full = [(rows, wide)] * 2 + [(rows, narrow)] * 4
    hbm = pl.BlockSpec(memory_space=pltpu.HBM)
    vmem = pl.BlockSpec(memory_space=pltpu.VMEM)
    scales = [((wide,), jnp.float32), ((narrow,), jnp.float32), ((narrow,), jnp.float32)]
    gathered = pl.pallas_call(
        functools.partial(kernel, n, pieces, turned),
        out_shape=[pltpu.VMEM((n * rows, width), jnp.bfloat16)]
        + [pltpu.VMEM(shape, dtype) for shape, dtype in scales],
        in_specs=[hbm] * 8,
        out_specs=[vmem] * 4,
        scratch_shapes=[
            tuple(pltpu.VMEM(shape, jnp.float32) for shape in full)
            + (pltpu.VMEM((rows,), jnp.float32),) * 2,
            pltpu.VMEM((rows, 128), jnp.float32),
            pltpu.VMEM((rows, 128), jnp.float32),
            pltpu.VMEM((rows, width), jnp.float32),
            pltpu.VMEM((n, width // 128, 128), jnp.float32),
            pltpu.VMEM((n // 2, width // 128, 128), jnp.float32),
            pltpu.VMEM((width // 128, 128), jnp.float32),
            pltpu.VMEM((width // 128, 128), jnp.float32),
            pltpu.VMEM((2, AHEAD, width), jnp.float32),
            pltpu.SemaphoreType.DMA((8,)),
            pltpu.SemaphoreType.DMA((5,)),
            pltpu.SemaphoreType.DMA((4,)),
            pltpu.SemaphoreType.REGULAR,
            pltpu.SemaphoreType.DMA((1,)),
            pltpu.SemaphoreType.DMA((4,)),
            pltpu.SemaphoreType.DMA((3 * steps + 2,)),
            pltpu.SemaphoreType.DMA((3 * steps + 1,)),
        ],
        compiler_params=pltpu.CompilerParams(
            collective_id=0, has_side_effects=True, vmem_limit_bytes=24 * 2**20
        ),
    )(
        *(
            pltpu.with_memory_space_constraint(x, pltpu.HBM)
            for x in (
                one_query,
                other_query,
                one_key,
                other_key,
                one_value,
                other_value,
                mix_share,
                norm_gain,
            )
        )
    )
    outs = [((n * rows, wide), jnp.bfloat16)] + [((n * rows, narrow), jnp.bfloat16)] * 2 + scales
    return pl.pallas_call(
        stored,
        out_shape=[pltpu.HBM(shape, dtype) for shape, dtype in outs],
        in_specs=[vmem] * 4,
        out_specs=[hbm] * 6,
        scratch_shapes=[pltpu.SemaphoreType.DMA((4,))],
        compiler_params=pltpu.CompilerParams(vmem_limit_bytes=2**20),
    )(*gathered)


def solution(mesh):
    placed = (
        P(("job", "shard"), "cols"),
        P(("job", "shard"), "cols"),
        P(("job", "shard"), "cols"),
        P(("job", "shard"), "cols"),
        P(("job", "shard"), "cols"),
        P(("job", "shard"), "cols"),
        P(("job", "shard")),
        P(("job", "shard")),
    )
    return jax.shard_map(
        shards,
        mesh=mesh,
        in_specs=placed,
        out_specs=(
            P("job", "cols"),
            P("job", "cols"),
            P("job", "cols"),
            P(("job", "cols")),
            P(("job", "cols")),
            P(("job", "cols")),
        ),
        check_vma=False,
    )
```
